256 devices in a mesh: seq: 64 (over x, z, core), head: 4 (over y).
Axes of the slice: x: 4, y: 4, z: 8, core: 2. Of those that a mesh axis runs over, the one named last changes fastest.
Arguments:
- stream: bfloat16 [32768, 5120], P('seq', 'head'), may hold values from -6 to 6
- gate_input: bfloat16 [32768, 5120], P('seq', 'head'), may hold values from -6 to 6
- in_coeff: bfloat16 [32768, 128], P('seq'), may hold values from -0.5 to 0.5
- out_coeff: bfloat16 [32768, 128], P('seq'), may hold values from -0.5 to 0.5
- step_raw: float32 [80, 32768], P('head', 'seq'), may hold values from -4 to 4
- step_bias: float32 [80], P('head'), may hold values from -1 to 1
- decay_rate: float32 [80], P('head'), may hold values from 3.0517578e-05 to 0.05
- skip_scale: float32 [80], P('head'), may hold values from 0.5 to 5
- norm_gain: float32 [5120], P('head'), may hold values from 0.1 to 1.9
- out_proj: bfloat16 [5120, 2560], P('head'), may hold values from -0.078125 to 0.078125
- doc_starts: int32 [128], replicated, may hold values from 0 to 32767, as said below
Outputs:
- layer_out: bfloat16 [32768, 2560], P(('seq', 'head'))
The draws below stay inside these ranges and needn't reach their ends.
Inputs may be any that keep to these rules, and one draw needn't show every extreme that they name: `doc_starts`: the first entry is 0, the last is 32767, and the entries strictly increase; entry i is the position where document i begins.
All inputs are finite; a program needn't handle non-finite values.
Results may differ from the reference program's by a relative error of at most 0.01.
Values may be sent and summed in bfloat16 or wider, within the bound.
No kernel may reach another device: no remote copies, remote signals or barrier semaphores. Data moves between devices by JAX's collectives and lax.ppermute only.
A program may use at most 128 MiB of HBM per device.

```python
import math
import jax
import jax.numpy as jnp
from jax import lax

D = 2560
HEADS = 80
HEAD_DIM = 64
STATE = 128
DI = 5120
BLOCK = 256
TOKENS = 32768
DOCS = 128
N_HEAD = 4


def draw_decay_rate(key, part):
    pick_key = jax.random.fold_in(key, 101)
    slow_key = jax.random.fold_in(key, 102)
    fast_key = jax.random.fold_in(key, 103)
    slow_share = 0.5
    slow_pick = jax.random.uniform(pick_key, (HEADS,), jnp.float32) < slow_share
    slow_rate = jnp.exp(jax.random.uniform(slow_key, (HEADS,), jnp.float32, 0.0, math.log(2.5))) / TOKENS
    fast_rate = jnp.exp(jax.random.uniform(fast_key, (HEADS,), jnp.float32, math.log(0.01), math.log(0.05)))
    return jnp.where(slow_pick, slow_rate, fast_rate).astype(jnp.float32)


def draw_skip_scale(key, part):
    noise_key = jax.random.fold_in(key, 201)
    ramp_line = 1.0 + 2.0 * jnp.arange(HEADS, dtype=jnp.float32) / max(HEADS - 1, 1)
    noise = jax.random.uniform(noise_key, (HEADS,), jnp.float32, 0.6, 1.4)
    return (ramp_line * noise).astype(jnp.float32)


def draw_doc_starts(key, part):
    quarter_span = TOKENS // 4
    cut_key = jax.random.fold_in(key, 301)
    shuffled = jax.random.permutation(cut_key, quarter_span) + quarter_span
    cuts = jnp.sort(shuffled[:DOCS - 2]).astype(jnp.int32)
    first_one = jnp.zeros((1,), jnp.int32)
    last_one = jnp.full((1,), TOKENS - 1, jnp.int32)
    return jnp.concatenate([first_one, cuts, last_one]).astype(jnp.int32)


def block_scale(key, dims, shards, least, top_value):
    def one(axis_at, blocks):
        heights = jax.random.uniform(jax.random.fold_in(jax.random.fold_in(key, 6), axis_at), (blocks,), jnp.float32, least / len(shards), top_value / len(shards))
        return jnp.repeat(jnp.exp(heights), dims[axis_at] // blocks).reshape((-1,) + (1,) * (len(dims) - axis_at - 1))

    level = one(*shards[0])
    for cut in shards[1:]:
        level = level * one(*cut)
    return level


def gaussian(key, extent, spread, limit, cuts=(), held_as=jnp.bfloat16):
    array = spread * jax.random.normal(key, extent, jnp.float32)
    if cuts:
        array = array * block_scale(key, extent, cuts, -0.22, 0.18)
    return jnp.clip(array, -limit, limit).astype(held_as)


def setup_inputs(seed: int = 0) -> dict:
    key_list = jax.random.split(jax.random.key(seed), 12)
    return {
        "stream": gaussian(key_list[0], (TOKENS, DI), 1.0, 6.0, ((0, 64), (1, 4))),
        "gate_input": gaussian(key_list[1], (TOKENS, DI), 1.0, 6.0, ((0, 64), (1, 4))),
        "in_coeff": gaussian(key_list[2], (TOKENS, STATE), STATE ** -0.5, 0.5, ((0, 64),)),
        "out_coeff": gaussian(key_list[3], (TOKENS, STATE), STATE ** -0.5, 0.5, ((0, 64),)),
        "step_raw": gaussian(key_list[4], (HEADS, TOKENS), 1.0, 4.0, ((0, 4), (1, 64)), jnp.float32),
        "step_bias": jnp.clip(jax.random.uniform(key_list[5], (HEADS,), jnp.float32, -1.0, 1.0) * block_scale(key_list[5], (HEADS,), ((0, 4),), -0.4, 0.0), -1.0, 1.0),
        "decay_rate": draw_decay_rate(jax.random.fold_in(key_list[11], 71), 0),
        "skip_scale": draw_skip_scale(jax.random.fold_in(key_list[11], 71), 0),
        "norm_gain": jnp.clip(1.0 + 0.18 * jax.random.normal(key_list[8], (DI,), jnp.float32), 0.1, 1.9),
        "out_proj": gaussian(key_list[9], (DI, D), DI ** -0.5, 0.078125, ((0, 4),)),
        "doc_starts": draw_doc_starts(jax.random.fold_in(key_list[11], 71), 0),
    }


EPSILON = 1e-05
HIGHEST = lax.Precision.HIGHEST

def block_pass(carry_state, block_piece):
    stream_blk, in_blk, out_blk, step_blk, log_blk, doc_blk, before = block_piece
    head_count = step_blk.shape[0]
    span = step_blk.shape[1]
    head_size = stream_blk.shape[1] // head_count
    index_row = lax.iota(jnp.int32, span)
    upper_ones = (index_row[:, None] <= index_row[None, :]).astype(jnp.float32)
    cumulative = jnp.dot(log_blk, upper_ones, precision=HIGHEST)
    last_cum = cumulative[:, -1]
    same_end = (doc_blk == doc_blk[-1]).astype(jnp.float32)
    end_weight = jnp.exp(jnp.minimum(last_cum[:, None] - cumulative, 0.0)) * step_blk * same_end[None, :]
    scaled_in = (end_weight[:, :, None] * in_blk.astype(jnp.float32)[None, :, :]).astype(jnp.bfloat16)
    values = stream_blk.reshape(span, head_count, head_size)
    fresh_state = jnp.einsum('hsn,shp->hnp', scaled_in.astype(jnp.float32), values.astype(jnp.float32), precision=HIGHEST)
    joined = doc_blk == before
    carry_gate = jnp.where(joined[-1], jnp.exp(last_cum), 0.0)
    new_state = carry_gate[:, None, None] * carry_state + fresh_state
    scores = jnp.dot(out_blk, in_blk.T, preferred_element_type=jnp.float32)
    live_pairs = (doc_blk[:, None] == doc_blk[None, :]) & (index_row[:, None] >= index_row[None, :])
    decay_pairs = jnp.where(live_pairs[None], jnp.exp(jnp.minimum(cumulative[:, :, None] - cumulative[:, None, :], 0.0)), 0.0)
    weights = (scores[None] * decay_pairs * step_blk[:, None, :]).astype(jnp.bfloat16)
    within = jnp.einsum('hts,shp->thp', weights.astype(jnp.float32), values.astype(jnp.float32), precision=HIGHEST)
    carried = jnp.einsum('tn,hnp->thp', out_blk.astype(jnp.float32), carry_state, precision=HIGHEST)
    factor = jnp.where(joined[None, :], jnp.exp(cumulative), 0.0)
    output = within + factor.T[:, :, None] * carried
    return (new_state, output)

def reference(stream, gate_input, in_coeff, out_coeff, step_raw, step_bias, decay_rate, skip_scale, norm_gain, out_proj, doc_starts):
    position = lax.iota(jnp.int32, TOKENS)
    doc_ids = lax.optimization_barrier(jnp.sum((doc_starts[None, :] <= position[:, None]).astype(jnp.int32), axis=1)) - 1
    step_size = jax.nn.softplus(step_raw + step_bias[:, None])
    log_decay = -step_size * decay_rate[:, None]
    block_count = TOKENS // BLOCK
    block_docs = doc_ids.reshape(block_count, BLOCK)
    block_before = jnp.concatenate([jnp.full((1,), -1, jnp.int32), block_docs[:-1, -1]])
    pieces = (stream.reshape(block_count, BLOCK, DI), in_coeff.reshape(block_count, BLOCK, STATE), out_coeff.reshape(block_count, BLOCK, STATE), step_size.reshape(HEADS, block_count, BLOCK).transpose(1, 0, 2), log_decay.reshape(HEADS, block_count, BLOCK).transpose(1, 0, 2), block_docs, block_before)
    zero_state = jnp.zeros((HEADS, STATE, HEAD_DIM), jnp.float32)
    last_state, outputs = lax.scan(block_pass, zero_state, pieces)
    ssm_out = outputs.reshape(TOKENS, HEADS, HEAD_DIM) + skip_scale[None, :, None] * stream.reshape(TOKENS, HEADS, HEAD_DIM).astype(jnp.float32)
    gated = ssm_out.reshape(TOKENS, DI) * jax.nn.silu(gate_input.astype(jnp.float32))
    scale_row = lax.rsqrt(lax.optimization_barrier(jnp.sum(gated * gated, axis=1)) / DI + EPSILON)
    hidden = (gated * scale_row[:, None] * norm_gain[None, :]).astype(jnp.bfloat16)
    group_width = DI // N_HEAD
    summed = jnp.zeros((TOKENS, D), jnp.float32)
    for group_index in range(N_HEAD):
        low = group_index * group_width
        part_sum = jnp.dot(hidden[:, low:low + group_width], out_proj[low:low + group_width, :], preferred_element_type=jnp.float32)
        summed = summed + lax.optimization_barrier(part_sum.astype(jnp.bfloat16)).astype(jnp.float32)
    return summed.astype(jnp.bfloat16)
```

```python
import functools

import jax
import jax.numpy as jnp
from jax import lax
from jax.experimental import pallas as pl
from jax.experimental.pallas import tpu as pltpu
from jax.sharding import Mesh
from jax.sharding import PartitionSpec as P

BLOCK = 256
SEQ = ("seq_0", "seq_1", "seq_2")
SEQ_HEAD = ("seq_0", "seq_1", "seq_2", "head")
EPSILON = 1e-05
F32 = jnp.float32
BF16 = jnp.bfloat16
PAD = 32
LANES = 128

VMEM_SPEC = pl.BlockSpec(memory_space=pltpu.VMEM)
SMEM_SPEC = pl.BlockSpec(memory_space=pltpu.SMEM)


def dot(a, b):
    return jnp.dot(a, b, preferred_element_type=F32)


def dot_first(a, b):
    return lax.dot_general(a, b, (((0,), (0,)), ((), ())), preferred_element_type=F32)


def dot_last(a, b):
    return lax.dot_general(a, b, (((1,), (1,)), ((), ())), preferred_element_type=F32)


def two_parts(value):
    high = value.astype(BF16)
    low = (value - high.astype(F32)).astype(BF16)
    return jnp.concatenate([high, low], axis=0)


def head_lanes(width, head_size):
    row = lax.broadcasted_iota(jnp.int32, (2 * PAD, width), 0)
    lane = lax.broadcasted_iota(jnp.int32, (2 * PAD, width), 1)
    head = jnp.where(row >= PAD, row - PAD, row)
    first = head * head_size
    return jnp.where((lane >= first) & (lane < first + head_size), 1.0, 0.0).astype(BF16)


def as_column(row, count):
    wide = jnp.broadcast_to(row, (count, row.shape[1]))
    i = lax.broadcasted_iota(jnp.int32, wide.shape, 0)
    j = lax.broadcasted_iota(jnp.int32, wide.shape, 1)
    return jnp.sum(jnp.where(i == j, wide, 0.0), axis=1, keepdims=True)


def as_row(column, width):
    wide = jnp.broadcast_to(column, (column.shape[0], width))
    i = lax.broadcasted_iota(jnp.int32, wide.shape, 0)
    j = lax.broadcasted_iota(jnp.int32, wide.shape, 1)
    return jnp.sum(jnp.where(i == j, wide, 0.0), axis=0, keepdims=True)


def docs_column(starts_row, first, count):
    position = first + lax.broadcasted_iota(jnp.int32, (count, starts_row.shape[1]), 0)
    hit = jnp.where(starts_row <= position, 1.0, 0.0)
    return jnp.sum(hit, axis=1, keepdims=True)


def docs_row(starts_row, first, count):
    position = first + lax.broadcasted_iota(jnp.int32, (count, starts_row.shape[1]), 0)
    hit = jnp.where(starts_row <= position, 1.0, 0.0).astype(BF16)
    ones = jnp.ones((8, starts_row.shape[1]), BF16)
    return dot_last(ones, hit)[:1, :]


def state_kernel(
    head_size,
    offset_ref,
    stream_ref,
    in_ref,
    step_ref,
    bias_ref,
    rate_ref,
    starts_ref,
    summary_ref,
    scaled_ref,
    first_ref,
    factor_ref,
):
    heads, rows = step_ref.shape
    width = stream_ref.shape[1]
    offset = offset_ref[0]
    starts = starts_ref[...]
    docs = docs_column(starts, offset, rows)
    before = jnp.max(docs_column(starts, offset - 1, 8)[:1, :], axis=0, keepdims=True)
    raw = step_ref[...] + as_column(bias_ref[...], heads)
    step = jnp.maximum(raw, 0.0) + jnp.log1p(jnp.exp(-jnp.abs(raw)))
    log_decay = -step * as_column(rate_ref[...], heads)
    i = lax.broadcasted_iota(jnp.int32, (BLOCK, BLOCK), 0)
    j = lax.broadcasted_iota(jnp.int32, (BLOCK, BLOCK), 1)
    upper = jnp.where(i <= j, 1.0, 0.0)
    into, out_of, half, last = [], [], [], []
    for block in range(rows // BLOCK):
        cut = slice(block * BLOCK, (block + 1) * BLOCK)
        cumulative = jnp.dot(
            log_decay[:, cut], upper, precision=lax.Precision.HIGHEST, preferred_element_type=F32
        )
        end = cumulative[:, BLOCK - 1 :]
        middle = 0.5 * end
        into.append(step[:, cut] * jnp.exp(middle - cumulative))
        out_of.append(jnp.exp(cumulative - middle))
        half.append(jnp.exp(middle))
        last.append(end)
    ends = [docs[(b + 1) * BLOCK - 1 : (b + 1) * BLOCK, :] for b in range(rows // BLOCK)]
    joined_0 = jnp.where(ends[0] == before, 1.0, 0.0)
    joined_1 = jnp.where(ends[1] == ends[0], 1.0, 0.0)
    gate_0 = joined_0 * jnp.exp(last[0])
    gate_1 = joined_1 * jnp.exp(last[1])
    link = joined_0 * joined_1 * jnp.exp(last[0] + last[1])
    lane = lax.broadcasted_iota(jnp.int32, (heads, LANES), 1)
    constants = jnp.where(lane == 0, half[0], 0.0)
    constants = jnp.where(lane == 1, half[1], constants)
    constants = jnp.where(lane == 2, gate_0, constants)
    constants = jnp.where(lane == 3, gate_1, constants)
    nothing = jnp.zeros((PAD - heads, rows + LANES), F32)
    spread = head_lanes(width, head_size)
    wide_in = jnp.concatenate([jnp.concatenate(into + [constants], axis=1), nothing], axis=0)
    wide_out = jnp.concatenate([jnp.concatenate(out_of + [constants], axis=1), nothing], axis=0)
    factor_ref[...] = two_parts(wide_out)
    per_lane = dot_first(two_parts(wide_in), spread)
    constant_rows = per_lane[rows : rows + 8, :]
    states = []
    for block in range(rows // BLOCK):
        cut = slice(block * BLOCK, (block + 1) * BLOCK)
        scaled = (stream_ref[cut, :].astype(F32) * per_lane[cut, :]).astype(BF16)
        scaled_ref[cut, :] = scaled
        to_end = jnp.where(docs[cut, :] == ends[block], in_ref[cut, :].astype(F32), 0.0)
        states.append(constant_rows[block : block + 1, :] * dot_first(to_end.astype(BF16), scaled))
    first_ref[...] = states[0]
    summary = constant_rows[3:4, :] * states[0] + states[1]
    high = link.astype(BF16).astype(F32)
    link_row = as_row(high, LANES) + pltpu.roll(as_row(link - high, LANES), PAD, 1)
    summary_ref[:, :width] = summary.astype(BF16)
    summary_ref[:, width:] = jnp.broadcast_to(link_row, (summary.shape[0], LANES)).astype(BF16)


def within_kernel(
    head_size,
    offset_ref,
    stream_ref,
    gate_ref,
    in_ref,
    out_ref,
    scaled_ref,
    factor_ref,
    skip_ref,
    starts_ref,
    base_ref,
    slope_ref,
):
    rows, width = stream_ref.shape
    heads = skip_ref.shape[1]
    offset = offset_ref[0]
    starts = starts_ref[...]
    docs = docs_column(starts, offset, rows)
    docs_across = docs_row(starts, offset, rows)
    spread = head_lanes(width, head_size)
    skip = jnp.concatenate(
        [as_column(skip_ref[...], heads), jnp.zeros((PAD - heads, 1), F32)], axis=0
    )
    skip_row = dot_first(two_parts(jnp.broadcast_to(skip, (PAD, LANES))), spread)[:1, :]
    i = lax.broadcasted_iota(jnp.int32, (BLOCK, BLOCK), 0)
    j = lax.broadcasted_iota(jnp.int32, (BLOCK, BLOCK), 1)
    for block in range(rows // BLOCK):
        cut = slice(block * BLOCK, (block + 1) * BLOCK)
        scores = dot_last(out_ref[cut, :], in_ref[cut, :])
        live = (i >= j) & (docs[cut, :] == docs_across[:, cut])
        weights = jnp.where(live, scores, 0.0).astype(BF16)
        per_lane = dot_first(factor_ref[:, cut], spread)
        within = dot(weights, scaled_ref[cut, :])
        value = per_lane * within + skip_row * stream_ref[cut, :].astype(F32)
        gate = gate_ref[cut, :].astype(F32)
        gate = gate / (1.0 + jnp.exp(-gate))
        base_ref[cut, :] = value * gate
        slope_ref[cut, :] = per_lane * gate


def scan_kernel(head_size, pieces_ref, before_ref):
    shards, rows, wide = pieces_ref.shape
    width = wide - LANES
    links = pieces_ref[:, 0, width:]
    lane = lax.broadcasted_iota(jnp.int32, (LANES, width), 0)
    spot = lax.broadcasted_iota(jnp.int32, (LANES, width), 1)
    head = jnp.where(lane >= PAD, lane - PAD, lane)
    first = head * head_size
    spread = jnp.where(
        (lane < 2 * PAD) & (spot >= first) & (spot < first + head_size), 1.0, 0.0
    ).astype(BF16)
    per_lane = dot(links, spread)
    state = jnp.zeros((rows, width), F32)
    for shard in range(shards):
        before_ref[shard] = state.astype(BF16)
        state = per_lane[shard : shard + 1, :] * state + pieces_ref[shard, :, :width].astype(F32)


def finish_kernel(
    head_size,
    offset_ref,
    blocks_ref,
    out_ref,
    before_ref,
    first_ref,
    factor_ref,
    base_ref,
    slope_ref,
    gain_ref,
    starts_ref,
    proj_ref,
    hidden_ref,
    squares_ref,
    send_a_ref,
    send_b_ref,
):
    rows, width = base_ref.shape
    offset = offset_ref[0]
    starts = starts_ref[...]
    docs = docs_column(starts, offset, rows)
    before = jnp.max(docs_column(starts, offset - 1, 8)[:1, :], axis=0, keepdims=True)
    spread = head_lanes(width, head_size)
    constant_rows = dot_first(factor_ref[:, rows:], spread)[:8, :]
    state = before_ref[...].astype(F32)
    gain = gain_ref[...]
    sums = []
    for block in range(rows // BLOCK):
        cut = slice(block * BLOCK, (block + 1) * BLOCK)
        joined = jnp.where(docs[cut, :] == before, out_ref[cut, :].astype(F32), 0.0).astype(BF16)
        carried = dot(joined, (constant_rows[block : block + 1, :] * state).astype(BF16))
        gated = base_ref[cut, :] + slope_ref[cut, :] * carried
        square = gated * gated
        total = square[:, :LANES]
        for lane in range(LANES, width, LANES):
            total = total + square[:, lane : lane + LANES]
        sums.append(total)
        hidden_ref[cut, :] = (gated * gain).astype(BF16)
        state = constant_rows[2:3, :] * state + first_ref[...]
        before = docs[(block + 1) * BLOCK - 1 : (block + 1) * BLOCK, :]
    flat = jnp.concatenate([jnp.sum(jnp.transpose(s), axis=0, keepdims=True) for s in sums], axis=1)
    squares_ref[...] = flat
    step = rows // 4
    half = proj_ref.shape[1] // 2
    for number, (send_ref, low) in enumerate(((send_a_ref, 0), (send_b_ref, half))):
        for part in range(2):
            block = blocks_ref[2 * number + part]
            piece = hidden_ref[pl.ds(block * step, step), :]
            send_ref[part * step : (part + 1) * step, :] = dot(
                piece, proj_ref[:, low : low + half]
            ).astype(BF16)


def keep_kernel(blocks_ref, hidden_ref, proj_ref, keep_a_ref, keep_b_ref):
    step = hidden_ref.shape[0] // 4
    half = proj_ref.shape[1] // 2
    for number, (keep_ref, low) in enumerate(((keep_a_ref, 0), (keep_b_ref, half))):
        for part in range(2):
            block = blocks_ref[4 + 2 * number + part]
            piece = hidden_ref[pl.ds(block * step, step), :]
            keep_ref[part * step : (part + 1) * step, :] = dot(
                piece, proj_ref[:, low : low + half]
            ).astype(BF16)


def middle_kernel(keep_a_ref, keep_b_ref, got_a_ref, got_b_ref, send_a_ref, send_b_ref):
    step = send_a_ref.shape[0]
    for keep_ref, got_ref, send_ref in (
        (keep_a_ref, got_a_ref, send_a_ref),
        (keep_b_ref, got_b_ref, send_b_ref),
    ):
        send_ref[...] = (
            keep_ref[step:, :].astype(F32) + got_ref[step:, :].astype(F32)
        ).astype(BF16)


def last_kernel(
    channels, squares_ref, keep_a_ref, keep_b_ref, got_a_ref, got_b_ref, far_a_ref, far_b_ref, out_ref
):
    step = far_a_ref.shape[0]
    half = far_a_ref.shape[1]
    mean = jnp.sum(squares_ref[...], axis=(0, 1))[None, :] / channels
    scale = as_column(lax.rsqrt(mean + EPSILON), step)
    for keep_ref, got_ref, far_ref, low in (
        (keep_a_ref, got_a_ref, far_a_ref, 0),
        (keep_b_ref, got_b_ref, far_b_ref, half),
    ):
        total = (
            keep_ref[:step, :].astype(F32) + got_ref[:step, :].astype(F32) + far_ref[...].astype(F32)
        )
        out_ref[:, low : low + half] = (total * scale).astype(BF16)


def call(kernel, out_shape, scalars, arrays, flops, name):
    single = not isinstance(out_shape, (tuple, list))
    return pl.pallas_call(
        kernel,
        out_shape=out_shape,
        in_specs=[SMEM_SPEC] * len(scalars) + [VMEM_SPEC] * len(arrays),
        out_specs=VMEM_SPEC if single else [VMEM_SPEC] * len(out_shape),
        cost_estimate=pl.CostEstimate(flops=flops, bytes_accessed=4_000_000, transcendentals=0),
        compiler_params=pltpu.CompilerParams(vmem_limit_bytes=48 * 1024 * 1024),
        name=name,
    )(*scalars, *arrays)


def local(
    total_channels,
    stream,
    gate_input,
    in_coeff,
    out_coeff,
    step_raw,
    step_bias,
    decay_rate,
    skip_scale,
    norm_gain,
    out_proj,
    doc_starts,
):
    rows, width = stream.shape
    heads = step_raw.shape[0]
    head_size = width // heads
    states = in_coeff.shape[1]
    model = out_proj.shape[1]
    shards = lax.axis_size(SEQ)
    y = lax.axis_index("head")
    offset = (lax.axis_index(SEQ) * rows).astype(jnp.int32)[None]
    starts = doc_starts[None, :]
    shape = jax.ShapeDtypeStruct
    summary, scaled, first, factor = call(
        functools.partial(state_kernel, head_size),
        [
            shape((states, width + LANES), BF16),
            shape((rows, width), BF16),
            shape((states, width), F32),
            shape((2 * PAD, rows + LANES), BF16),
        ],
        [offset],
        [stream, in_coeff, step_raw, step_bias[None], decay_rate[None], starts],
        2_000_000_000,
        "state",
    )
    pieces = lax.all_to_all(
        summary.reshape(shards, states // shards, width + LANES), SEQ, 0, 0, tiled=True
    )
    base, slope = call(
        functools.partial(within_kernel, head_size),
        [shape((rows, width), F32), shape((rows, width), F32)],
        [offset],
        [stream, gate_input, in_coeff, out_coeff, scaled, factor, skip_scale[None], starts],
        4_000_000_000,
        "within",
    )
    prior = call(
        functools.partial(scan_kernel, head_size),
        shape((shards, states // shards, width), BF16),
        [],
        [pieces],
        1_000_000_000,
        "scan",
    )
    incoming = lax.all_to_all(prior, SEQ, 0, 0, tiled=True).reshape(states, width)
    one, two, three = y ^ 1, y ^ 2, y ^ 3
    blocks = jnp.stack([one, two, three, two, y, three, y, one]).astype(jnp.int32)
    step = rows // 4
    half = model // 2
    hidden, squares, send_a, send_b = call(
        functools.partial(finish_kernel, head_size),
        [
            shape((rows, width), BF16),
            shape((1, rows), F32),
            shape((2 * step, half), BF16),
            shape((2 * step, half), BF16),
        ],
        [offset, blocks],
        [out_coeff, incoming, first, factor, base, slope, norm_gain[None], starts, out_proj],
        4_000_000_000,
        "finish",
    )
    pair_1 = [(i, i ^ 1) for i in range(4)]
    pair_3 = [(i, i ^ 3) for i in range(4)]
    all_squares = lax.all_to_all(squares.reshape(4, 1, step), "head", 0, 0, tiled=True)
    got_a = lax.ppermute(send_a, "head", pair_1)
    got_b = lax.ppermute(send_b, "head", pair_3)
    keep_a, keep_b = call(
        keep_kernel,
        [shape((2 * step, half), BF16), shape((2 * step, half), BF16)],
        [blocks],
        [hidden, out_proj],
        2_000_000_000,
        "keep",
    )
    more_a, more_b = call(
        middle_kernel,
        [shape((step, half), BF16), shape((step, half), BF16)],
        [],
        [keep_a, keep_b, got_a, got_b],
        1_000_000_000,
        "middle",
    )
    far_a = lax.ppermute(more_a, "head", pair_3)
    far_b = lax.ppermute(more_b, "head", pair_1)
    return call(
        functools.partial(last_kernel, total_channels),
        shape((step, model), BF16),
        [],
        [all_squares, keep_a, keep_b, got_a, got_b, far_a, far_b],
        1_000_000_000,
        "last",
    )


def solution(mesh):
    split = Mesh(
        mesh.devices.reshape(4, 8, 2, mesh.shape["head"]), ("seq_0", "seq_1", "seq_2", "head")
    )
    in_specs = (
        P(SEQ, "head"),
        P(SEQ, "head"),
        P(SEQ, None),
        P(SEQ, None),
        P("head", SEQ),
        P("head"),
        P("head"),
        P("head"),
        P("head"),
        P("head", None),
        P(),
    )
    out_specs = P(SEQ_HEAD, None)

    def whole(*args):
        step = functools.partial(local, float(args[0].shape[1]))
        return jax.shard_map(
            step, mesh=split, in_specs=in_specs, out_specs=out_specs, check_vma=False
        )(*args)

    return whole
```

```python
import functools

import jax
import jax.numpy as jnp
from jax import lax
from jax.experimental import pallas as pl
from jax.experimental.pallas import tpu as pltpu
from jax.sharding import Mesh
from jax.sharding import PartitionSpec as P

BLOCK = 256
SEQ = ("seq_0", "seq_1", "seq_2")
SEQ_HEAD = ("seq_0", "seq_1", "seq_2", "head")
EPSILON = 1e-05
F32 = jnp.float32
BF16 = jnp.bfloat16
PAD = 32
LANES = 128
FULL = 67_043_328 / 1024**2

VMEM_SPEC = pl.BlockSpec(memory_space=pltpu.VMEM)
SMEM_SPEC = pl.BlockSpec(memory_space=pltpu.SMEM)
HBM_SPEC = pl.BlockSpec(memory_space=pltpu.HBM)


def dot(a, b):
    return jnp.dot(a, b, preferred_element_type=F32)


def dot_first(a, b):
    return lax.dot_general(a, b, (((0,), (0,)), ((), ())), preferred_element_type=F32)


def dot_last(a, b):
    return lax.dot_general(a, b, (((1,), (1,)), ((), ())), preferred_element_type=F32)


def two_parts(value):
    high = value.astype(BF16)
    low = (value - high.astype(F32)).astype(BF16)
    return jnp.concatenate([high, low], axis=0)


def head_lanes(width, head_size):
    row = lax.broadcasted_iota(jnp.int32, (2 * PAD, width), 0)
    lane = lax.broadcasted_iota(jnp.int32, (2 * PAD, width), 1)
    head = jnp.where(row >= PAD, row - PAD, row)
    first = head * head_size
    return jnp.where((lane >= first) & (lane < first + head_size), 1.0, 0.0).astype(BF16)


def as_column(row, count):
    wide = jnp.broadcast_to(row, (count, row.shape[1]))
    i = lax.broadcasted_iota(jnp.int32, wide.shape, 0)
    j = lax.broadcasted_iota(jnp.int32, wide.shape, 1)
    return jnp.sum(jnp.where(i == j, wide, 0.0), axis=1, keepdims=True)


def as_row(column, width):
    wide = jnp.broadcast_to(column, (column.shape[0], width))
    i = lax.broadcasted_iota(jnp.int32, wide.shape, 0)
    j = lax.broadcasted_iota(jnp.int32, wide.shape, 1)
    return jnp.sum(jnp.where(i == j, wide, 0.0), axis=0, keepdims=True)


def docs_column(starts_row, first, count):
    position = first + lax.broadcasted_iota(jnp.int32, (count, starts_row.shape[1]), 0)
    hit = jnp.where(starts_row <= position, 1.0, 0.0)
    return jnp.sum(hit, axis=1, keepdims=True)


def docs_row(starts_row, first, count):
    position = first + lax.broadcasted_iota(jnp.int32, (count, starts_row.shape[1]), 0)
    hit = jnp.where(starts_row <= position, 1.0, 0.0).astype(BF16)
    ones = jnp.ones((8, starts_row.shape[1]), BF16)
    return dot_last(ones, hit)[:1, :]


def state_kernel(
    head_size,
    offset_ref,
    y_ref,
    stream_hbm,
    in_hbm,
    step_hbm,
    bias_hbm,
    rate_hbm,
    starts_hbm,
    summary_ref,
    into_ref,
    factor_ref,
    stream_ref,
    in_ref,
    step_ref,
    bias_ref,
    rate_ref,
    starts_ref,
    arrived,
):
    pairs = (
        (step_hbm, step_ref),
        (bias_hbm, bias_ref),
        (rate_hbm, rate_ref),
        (starts_hbm, starts_ref),
        (in_hbm, in_ref),
        (stream_hbm, stream_ref),
    )
    copies = [
        pltpu.make_async_copy(source, target, arrived.at[number])
        for number, (source, target) in enumerate(pairs)
    ]
    for copy in copies:
        copy.start()
    for copy in copies[:4]:
        copy.wait()
    heads, rows = step_ref.shape
    width = stream_ref.shape[1]
    offset = offset_ref[0]
    starts = starts_ref[...]
    docs = docs_column(starts, offset, rows)
    before = jnp.max(docs_column(starts, offset - 1, 8)[:1, :], axis=0, keepdims=True)
    raw = step_ref[...] + as_column(bias_ref[...], heads)
    step = jnp.maximum(raw, 0.0) + jnp.log1p(jnp.exp(-jnp.abs(raw)))
    log_decay = -step * as_column(rate_ref[...], heads)
    i = lax.broadcasted_iota(jnp.int32, (BLOCK, BLOCK), 0)
    j = lax.broadcasted_iota(jnp.int32, (BLOCK, BLOCK), 1)
    upper = jnp.where(i <= j, 1.0, 0.0)
    into, out_of, half, last = [], [], [], []
    for block in range(rows // BLOCK):
        cut = slice(block * BLOCK, (block + 1) * BLOCK)
        cumulative = jnp.dot(
            log_decay[:, cut], upper, precision=lax.Precision.HIGHEST, preferred_element_type=F32
        )
        end = cumulative[:, BLOCK - 1 :]
        middle = 0.5 * end
        into.append(step[:, cut] * jnp.exp(middle - cumulative))
        out_of.append(jnp.exp(cumulative - middle))
        half.append(jnp.exp(middle))
        last.append(end)
    ends = [docs[(b + 1) * BLOCK - 1 : (b + 1) * BLOCK, :] for b in range(rows // BLOCK)]
    joined_0 = jnp.where(ends[0] == before, 1.0, 0.0)
    joined_1 = jnp.where(ends[1] == ends[0], 1.0, 0.0)
    gate_0 = joined_0 * jnp.exp(last[0])
    gate_1 = joined_1 * jnp.exp(last[1])
    link = joined_0 * joined_1 * jnp.exp(last[0] + last[1])
    lane = lax.broadcasted_iota(jnp.int32, (heads, LANES), 1)
    constants = jnp.where(lane == 0, half[0], 0.0)
    constants = jnp.where(lane == 1, half[1], constants)
    constants = jnp.where(lane == 2, gate_0, constants)
    constants = jnp.where(lane == 3, gate_1, constants)
    nothing = jnp.zeros((PAD - heads, rows + LANES), F32)
    spread = head_lanes(width, head_size)
    wide_in = jnp.concatenate([jnp.concatenate(into + [constants], axis=1), nothing], axis=0)
    wide_out = jnp.concatenate([jnp.concatenate(out_of + [constants], axis=1), nothing], axis=0)
    factor_ref[...] = two_parts(wide_out)
    into_parts = two_parts(wide_in)
    into_ref[...] = into_parts
    per_lane = dot_first(into_parts, spread)
    constant_rows = per_lane[rows : rows + 8, :]
    for copy in copies[4:]:
        copy.wait()
    states = []
    for block in range(rows // BLOCK):
        cut = slice(block * BLOCK, (block + 1) * BLOCK)
        scaled = (stream_ref[cut, :].astype(F32) * per_lane[cut, :]).astype(BF16)
        to_end = jnp.where(docs[cut, :] == ends[block], in_ref[cut, :].astype(F32), 0.0)
        states.append(constant_rows[block : block + 1, :] * dot_first(to_end.astype(BF16), scaled))
    summary = constant_rows[3:4, :] * states[0] + states[1]
    high = link.astype(BF16).astype(F32)
    link_row = as_row(high, LANES) + pltpu.roll(as_row(link - high, LANES), PAD, 1)
    whole = jnp.concatenate(
        [summary, jnp.broadcast_to(link_row, (summary.shape[0], LANES))], axis=1
    ).astype(BF16)
    summary_ref[...] = whole.reshape(summary_ref.shape)


def within_kernel(
    head_size,
    offset_ref,
    stream_ref,
    gate_ref,
    in_ref,
    out_ref,
    into_ref,
    factor_ref,
    skip_ref,
    starts_ref,
    base_ref,
    slope_ref,
    first_ref,
):
    rows, width = stream_ref.shape
    heads = skip_ref.shape[1]
    offset = offset_ref[0]
    starts = starts_ref[...]
    docs = docs_column(starts, offset, rows)
    docs_across = docs_row(starts, offset, rows)
    spread = head_lanes(width, head_size)
    skip = jnp.concatenate(
        [as_column(skip_ref[...], heads), jnp.zeros((PAD - heads, 1), F32)], axis=0
    )
    skip_row = dot_first(two_parts(jnp.broadcast_to(skip, (PAD, LANES))), spread)[:1, :]
    i = lax.broadcasted_iota(jnp.int32, (BLOCK, BLOCK), 0)
    j = lax.broadcasted_iota(jnp.int32, (BLOCK, BLOCK), 1)
    constant_rows = dot_first(into_ref[:, rows:], spread)[:8, :]
    for block in range(rows // BLOCK):
        cut = slice(block * BLOCK, (block + 1) * BLOCK)
        scaled = stream_ref[cut, :].astype(F32) * dot_first(into_ref[:, cut], spread)
        scaled = scaled.astype(BF16)
        if block == 0:
            end = docs[BLOCK - 1 : BLOCK, :]
            to_end = jnp.where(docs[cut, :] == end, in_ref[cut, :].astype(F32), 0.0)
            first_ref[...] = constant_rows[:1, :] * dot_first(to_end.astype(BF16), scaled)
        scores = dot_last(out_ref[cut, :], in_ref[cut, :])
        live = (i >= j) & (docs[cut, :] == docs_across[:, cut])
        weights = jnp.where(live, scores, 0.0).astype(BF16)
        per_lane = dot_first(factor_ref[:, cut], spread)
        within = dot(weights, scaled)
        value = per_lane * within + skip_row * stream_ref[cut, :].astype(F32)
        gate = gate_ref[cut, :].astype(F32)
        gate = gate / (1.0 + jnp.exp(-gate))
        base_ref[cut, :] = value * gate
        slope_ref[cut, :] = per_lane * gate


def scan_kernel(head_size, pieces_ref, before_ref):
    shards, rows, wide = pieces_ref.shape
    width = wide - LANES
    links = pieces_ref[:, 0, width:]
    lane = lax.broadcasted_iota(jnp.int32, (LANES, width), 0)
    spot = lax.broadcasted_iota(jnp.int32, (LANES, width), 1)
    head = jnp.where(lane >= PAD, lane - PAD, lane)
    first = head * head_size
    spread = jnp.where(
        (lane < 2 * PAD) & (spot >= first) & (spot < first + head_size), 1.0, 0.0
    ).astype(BF16)
    per_lane = dot(links, spread)
    state = jnp.zeros((rows, width), F32)
    for shard in range(shards):
        before_ref[shard] = state.astype(BF16)
        state = per_lane[shard : shard + 1, :] * state + pieces_ref[shard, :, :width].astype(F32)


def with_squares(piece, squares):
    width = piece.shape[1]
    high = squares.astype(BF16).astype(F32)
    row = jnp.concatenate(
        [high, squares - high, jnp.zeros((1, width - 2 * squares.shape[1]), F32)], axis=1
    )
    return jnp.concatenate(
        [piece.astype(BF16), jnp.broadcast_to(row, (8, width)).astype(BF16)], axis=0
    )


def squares_of(got_ref, step):
    row = got_ref[step:, :].astype(F32)[:1, :]
    return row[:, :step] + row[:, step : 2 * step]


def finish_kernel(
    head_size,
    offset_ref,
    out_ref,
    before_ref,
    first_ref,
    factor_ref,
    base_ref,
    slope_ref,
    gain_ref,
    starts_ref,
    hidden_ref,
    squares_ref,
):
    rows, width = base_ref.shape
    offset = offset_ref[0]
    starts = starts_ref[...]
    docs = docs_column(starts, offset, rows)
    before = jnp.max(docs_column(starts, offset - 1, 8)[:1, :], axis=0, keepdims=True)
    spread = head_lanes(width, head_size)
    constant_rows = dot_first(factor_ref[:, rows:], spread)[:8, :]
    state = before_ref[...].reshape(-1, width).astype(F32)
    gain = gain_ref[...].reshape(1, width)
    step = rows // 4
    for block in range(rows // BLOCK):
        cut = slice(block * BLOCK, (block + 1) * BLOCK)
        joined = jnp.where(docs[cut, :] == before, out_ref[cut, :].astype(F32), 0.0).astype(BF16)
        carried = dot(joined, (constant_rows[block : block + 1, :] * state).astype(BF16))
        gated = base_ref[cut, :] + slope_ref[cut, :] * carried
        square = gated * gated
        total = square[:, :LANES]
        for lane in range(LANES, width, LANES):
            total = total + square[:, lane : lane + LANES]
        for part in range(BLOCK // step):
            piece = total[part * step : (part + 1) * step, :]
            number = block * (BLOCK // step) + part
            squares_ref[number : number + 1, :] = jnp.sum(
                jnp.transpose(piece), axis=0, keepdims=True
            )
        hidden_ref[cut, :] = (gated * gain).astype(BF16)
        state = constant_rows[2:3, :] * state + first_ref[...]
        before = docs[(block + 1) * BLOCK - 1 : (block + 1) * BLOCK, :]


def far_kernel(y_ref, hidden_ref, proj_ref, squares_ref, send_a_ref, send_b_ref):
    step = hidden_ref.shape[0] // 4
    half = proj_ref.shape[1] // 2
    far = y_ref[0] ^ 2
    piece = hidden_ref[pl.ds(far * step, step), :]
    send_a_ref[...] = with_squares(
        dot(piece, proj_ref[:, :half]), squares_ref[pl.ds(far, 1), :]
    )
    send_b_ref[...] = dot(piece, proj_ref[:, half:]).astype(BF16)


def near_kernel(y_ref, hidden_ref, proj_ref, squares_ref, send_a_ref, send_b_ref):
    step = hidden_ref.shape[0] // 4
    half = proj_ref.shape[1] // 2
    one, three = y_ref[0] ^ 1, y_ref[0] ^ 3
    send_a_ref[...] = with_squares(
        dot(hidden_ref[pl.ds(one * step, step), :], proj_ref[:, :half]),
        squares_ref[pl.ds(one, 1), :],
    )
    send_b_ref[...] = dot(
        hidden_ref[pl.ds(three * step, step), :], proj_ref[:, half:]
    ).astype(BF16)


def keep_kernel(y_ref, hidden_ref, proj_ref, own_ref, via_a_ref, via_b_ref):
    step = hidden_ref.shape[0] // 4
    half = proj_ref.shape[1] // 2
    one, three = y_ref[0] ^ 1, y_ref[0] ^ 3
    via_a_ref[...] = dot(hidden_ref[pl.ds(three * step, step), :], proj_ref[:, :half])
    via_b_ref[...] = dot(hidden_ref[pl.ds(one * step, step), :], proj_ref[:, half:])
    own_ref[...] = dot(hidden_ref[pl.ds(y_ref[0] * step, step), :], proj_ref[...])


def middle_kernel(
    y_ref, squares_ref, via_a_ref, via_b_ref, got_a_ref, got_b_ref, send_a_ref, send_b_ref
):
    step = via_a_ref.shape[0]
    squares = squares_ref[pl.ds(y_ref[0] ^ 3, 1), :] + squares_of(got_a_ref, step)
    send_a_ref[...] = with_squares(via_a_ref[...] + got_a_ref[:step, :].astype(F32), squares)
    send_b_ref[...] = (via_b_ref[...] + got_b_ref[...].astype(F32)).astype(BF16)


def last_kernel(
    channels,
    y_ref,
    squares_ref,
    own_ref,
    near_a_ref,
    near_b_ref,
    far_a_ref,
    far_b_ref,
    out_ref,
):
    step, model = own_ref.shape
    half = model // 2
    squares = squares_ref[pl.ds(y_ref[0], 1), :]
    squares = squares + squares_of(near_a_ref, step) + squares_of(far_a_ref, step)
    scale = as_column(lax.rsqrt(squares / channels + EPSILON), step)
    for near_ref, far_ref, low in ((near_a_ref, far_a_ref, 0), (near_b_ref, far_b_ref, half)):
        total = (
            own_ref[:, low : low + half]
            + near_ref[:step, :].astype(F32)
            + far_ref[:step, :].astype(F32)
        )
        out_ref[:, low : low + half] = (total * scale).astype(BF16)


def call(kernel, out_shape, scalars, arrays, flops, limit, scratch=()):
    single = not isinstance(out_shape, (tuple, list))
    space = HBM_SPEC if scratch else VMEM_SPEC
    return pl.pallas_call(
        kernel,
        out_shape=out_shape,
        in_specs=[SMEM_SPEC] * len(scalars) + [space] * len(arrays),
        out_specs=VMEM_SPEC if single else [VMEM_SPEC] * len(out_shape),
        scratch_shapes=scratch,
        cost_estimate=pl.CostEstimate(flops=flops, bytes_accessed=4_000_000, transcendentals=0),
        compiler_params=pltpu.CompilerParams(vmem_limit_bytes=int(limit * 1024**2)),
    )(*scalars, *arrays)


def local(
    total_channels,
    stream,
    gate_input,
    in_coeff,
    out_coeff,
    step_raw,
    step_bias,
    decay_rate,
    skip_scale,
    norm_gain,
    out_proj,
    doc_starts,
):
    rows, width = stream.shape
    heads = step_raw.shape[0]
    head_size = width // heads
    states = in_coeff.shape[1]
    model = out_proj.shape[1]
    shards = lax.axis_size(SEQ)
    y = lax.axis_index("head").astype(jnp.int32)[None]
    offset = (lax.axis_index(SEQ) * rows).astype(jnp.int32)[None]
    starts = doc_starts[None, :]
    shape = jax.ShapeDtypeStruct
    arrays = [stream, in_coeff, step_raw, step_bias[None], decay_rate[None], starts]
    summary, into, factor = call(
        functools.partial(state_kernel, head_size),
        [
            shape((shards, states // shards, width + LANES), BF16),
            shape((2 * PAD, rows + LANES), BF16),
            shape((2 * PAD, rows + LANES), BF16),
        ],
        [offset, y],
        arrays,
        2_000_000_000,
        FULL,
        [pltpu.VMEM(a.shape, a.dtype) for a in arrays] + [pltpu.SemaphoreType.DMA((len(arrays),))],
    )
    pieces = lax.all_to_all(summary, SEQ, 0, 0, tiled=True)
    base, slope, first = call(
        functools.partial(within_kernel, head_size),
        [
            shape((rows, width), F32),
            shape((rows, width), F32),
            shape((states, width), F32),
        ],
        [offset],
        [stream, gate_input, in_coeff, out_coeff, into, factor, skip_scale[None], starts],
        4_000_000_000,
        FULL,
    )
    prior = call(
        functools.partial(scan_kernel, head_size),
        shape((shards, states // shards, width), BF16),
        [],
        [pieces],
        10_000_000_000,
        8,
    )
    incoming = lax.all_to_all(prior, SEQ, 0, 0, tiled=True)
    step = rows // 4
    half = model // 2
    hidden, squares = call(
        functools.partial(finish_kernel, head_size),
        [shape((rows, width), BF16), shape((4, step), F32)],
        [offset],
        [out_coeff, incoming, first, factor, base, slope, norm_gain, starts],
        4_000_000_000,
        22,
    )
    send_a, send_b = call(
        far_kernel,
        [shape((step + 8, half), BF16), shape((step, half), BF16)],
        [y],
        [hidden, out_proj, squares],
        1_000_000_000,
        16,
    )
    pair_1 = [(i, i ^ 1) for i in range(4)]
    pair_3 = [(i, i ^ 3) for i in range(4)]
    got_a = lax.ppermute(send_a, "head", pair_1)
    got_b = lax.ppermute(send_b, "head", pair_3)
    send_a, send_b = call(
        near_kernel,
        [shape((step + 8, half), BF16), shape((step, half), BF16)],
        [y],
        [hidden, out_proj, squares],
        1_000_000_000,
        16,
    )
    near_a = lax.ppermute(send_a, "head", pair_1)
    near_b = lax.ppermute(send_b, "head", pair_3)
    own, via_a, via_b = call(
        keep_kernel,
        [shape((step, model), F32), shape((step, half), F32), shape((step, half), F32)],
        [y],
        [hidden, out_proj],
        2_000_000_000,
        16,
    )
    send_a, send_b = call(
        middle_kernel,
        [shape((step + 8, half), BF16), shape((step, half), BF16)],
        [y],
        [squares, via_a, via_b, got_a, got_b],
        1_000_000_000,
        8,
    )
    far_a = lax.ppermute(send_a, "head", pair_3)
    far_b = lax.ppermute(send_b, "head", pair_1)
    return call(
        functools.partial(last_kernel, total_channels),
        shape((step, model), BF16),
        [y],
        [squares, own, near_a, near_b, far_a, far_b],
        1_000_000_000,
        8,
    )


def solution(mesh):
    split = Mesh(
        mesh.devices.reshape(4, 8, 2, mesh.shape["head"]), ("seq_0", "seq_1", "seq_2", "head")
    )
    in_specs = (
        P(SEQ, "head"),
        P(SEQ, "head"),
        P(SEQ, None),
        P(SEQ, None),
        P("head", SEQ),
        P("head"),
        P("head"),
        P("head"),
        P("head"),
        P("head", None),
        P(),
    )
    out_specs = P(SEQ_HEAD, None)

    def whole(*args):
        step = functools.partial(local, float(args[0].shape[1]))
        return jax.shard_map(
            step, mesh=split, in_specs=in_specs, out_specs=out_specs, check_vma=False
        )(*args)

    return whole
```

```python
import functools

import jax
import jax.numpy as jnp
from jax import lax
from jax.experimental import pallas as pl
from jax.experimental.pallas import tpu as pltpu
from jax.sharding import Mesh
from jax.sharding import PartitionSpec as P

BLOCK = 256
SEQ = ("seq_0", "seq_1", "seq_2")
CHIPS = ("seq_0", "seq_1")
SEQ_HEAD = ("seq_0", "seq_1", "seq_2", "head")
EPSILON = 1e-05
F32 = jnp.float32
BF16 = jnp.bfloat16
PAD = 32
LANES = 128
FULL = 67_043_328 / 1024**2

VMEM_SPEC = pl.BlockSpec(memory_space=pltpu.VMEM)
SMEM_SPEC = pl.BlockSpec(memory_space=pltpu.SMEM)
HBM_SPEC = pl.BlockSpec(memory_space=pltpu.HBM)


def dot(a, b):
    return jnp.dot(a, b, preferred_element_type=F32)


def dot_first(a, b):
    return lax.dot_general(a, b, (((0,), (0,)), ((), ())), preferred_element_type=F32)


def dot_last(a, b):
    return lax.dot_general(a, b, (((1,), (1,)), ((), ())), preferred_element_type=F32)


def two_parts(value):
    high = value.astype(BF16)
    low = (value - high.astype(F32)).astype(BF16)
    return jnp.concatenate([high, low], axis=0)


def head_lanes(width, head_size):
    row = lax.broadcasted_iota(jnp.int32, (2 * PAD, width), 0)
    lane = lax.broadcasted_iota(jnp.int32, (2 * PAD, width), 1)
    head = jnp.where(row >= PAD, row - PAD, row)
    first = head * head_size
    return jnp.where((lane >= first) & (lane < first + head_size), 1.0, 0.0).astype(BF16)


def as_column(row, count):
    wide = jnp.broadcast_to(row, (count, row.shape[1]))
    i = lax.broadcasted_iota(jnp.int32, wide.shape, 0)
    j = lax.broadcasted_iota(jnp.int32, wide.shape, 1)
    return jnp.sum(jnp.where(i == j, wide, 0.0), axis=1, keepdims=True)


def as_row(column, width):
    wide = jnp.broadcast_to(column, (column.shape[0], width))
    i = lax.broadcasted_iota(jnp.int32, wide.shape, 0)
    j = lax.broadcasted_iota(jnp.int32, wide.shape, 1)
    return jnp.sum(jnp.where(i == j, wide, 0.0), axis=0, keepdims=True)


def docs_column(starts_row, first, count):
    position = first + lax.broadcasted_iota(jnp.int32, (count, starts_row.shape[1]), 0)
    hit = jnp.where(starts_row <= position, 1.0, 0.0)
    return jnp.sum(hit, axis=1, keepdims=True)


def docs_row(starts_row, first, count):
    position = first + lax.broadcasted_iota(jnp.int32, (count, starts_row.shape[1]), 0)
    hit = jnp.where(starts_row <= position, 1.0, 0.0).astype(BF16)
    ones = jnp.ones((8, starts_row.shape[1]), BF16)
    return dot_last(ones, hit)[:1, :]


def state_kernel(
    head_size,
    offset_ref,
    y_ref,
    core_ref,
    stream_hbm,
    in_hbm,
    step_hbm,
    bias_hbm,
    rate_hbm,
    starts_hbm,
    summary_ref,
    into_ref,
    factor_ref,
    stream_ref,
    in_ref,
    step_ref,
    bias_ref,
    rate_ref,
    starts_ref,
    arrived,
):
    pairs = (
        (step_hbm, step_ref),
        (bias_hbm, bias_ref),
        (rate_hbm, rate_ref),
        (starts_hbm, starts_ref),
        (in_hbm, in_ref),
        (stream_hbm, stream_ref),
    )
    copies = [
        pltpu.make_async_copy(source, target, arrived.at[number])
        for number, (source, target) in enumerate(pairs)
    ]
    for copy in copies:
        copy.start()
    for copy in copies[:4]:
        copy.wait()
    heads, rows = step_ref.shape
    width = stream_ref.shape[1]
    offset = offset_ref[0]
    starts = starts_ref[...]
    docs = docs_column(starts, offset, rows)
    before = jnp.max(docs_column(starts, offset - 1, 8)[:1, :], axis=0, keepdims=True)
    raw = step_ref[...] + as_column(bias_ref[...], heads)
    step = jnp.maximum(raw, 0.0) + jnp.log1p(jnp.exp(-jnp.abs(raw)))
    log_decay = -step * as_column(rate_ref[...], heads)
    i = lax.broadcasted_iota(jnp.int32, (BLOCK, BLOCK), 0)
    j = lax.broadcasted_iota(jnp.int32, (BLOCK, BLOCK), 1)
    upper = jnp.where(i <= j, 1.0, 0.0)
    into, out_of, half, last = [], [], [], []
    for block in range(rows // BLOCK):
        cut = slice(block * BLOCK, (block + 1) * BLOCK)
        cumulative = jnp.dot(
            log_decay[:, cut], upper, precision=lax.Precision.HIGHEST, preferred_element_type=F32
        )
        end = cumulative[:, BLOCK - 1 :]
        middle = 0.5 * end
        into.append(step[:, cut] * jnp.exp(middle - cumulative))
        out_of.append(jnp.exp(cumulative - middle))
        half.append(jnp.exp(middle))
        last.append(end)
    ends = [docs[(b + 1) * BLOCK - 1 : (b + 1) * BLOCK, :] for b in range(rows // BLOCK)]
    joined_0 = jnp.where(ends[0] == before, 1.0, 0.0)
    joined_1 = jnp.where(ends[1] == ends[0], 1.0, 0.0)
    gate_0 = joined_0 * jnp.exp(last[0])
    gate_1 = joined_1 * jnp.exp(last[1])
    link = joined_0 * joined_1 * jnp.exp(last[0] + last[1])
    lane = lax.broadcasted_iota(jnp.int32, (heads, LANES), 1)
    constants = jnp.where(lane == 0, half[0], 0.0)
    constants = jnp.where(lane == 1, half[1], constants)
    constants = jnp.where(lane == 2, gate_0, constants)
    constants = jnp.where(lane == 3, gate_1, constants)
    nothing = jnp.zeros((PAD - heads, rows + LANES), F32)
    spread = head_lanes(width, head_size)
    wide_in = jnp.concatenate([jnp.concatenate(into + [constants], axis=1), nothing], axis=0)
    wide_out = jnp.concatenate([jnp.concatenate(out_of + [constants], axis=1), nothing], axis=0)
    factor_ref[...] = two_parts(wide_out)
    into_parts = two_parts(wide_in)
    into_ref[...] = into_parts
    per_lane = dot_first(into_parts, spread)
    constant_rows = per_lane[rows : rows + 8, :]
    for copy in copies[4:]:
        copy.wait()
    states = []
    for block in range(rows // BLOCK):
        cut = slice(block * BLOCK, (block + 1) * BLOCK)
        scaled = (stream_ref[cut, :].astype(F32) * per_lane[cut, :]).astype(BF16)
        to_end = jnp.where(docs[cut, :] == ends[block], in_ref[cut, :].astype(F32), 0.0)
        states.append(constant_rows[block : block + 1, :] * dot_first(to_end.astype(BF16), scaled))
    summary = constant_rows[3:4, :] * states[0] + states[1]
    high = link.astype(BF16).astype(F32)
    link_row = as_row(high, LANES) + pltpu.roll(as_row(link - high, LANES), PAD, 1)
    whole = jnp.concatenate(
        [summary, jnp.broadcast_to(link_row, (summary.shape[0], LANES))], axis=1
    ).astype(BF16)
    summary_ref[...] = whole


def within_kernel(
    head_size,
    offset_ref,
    stream_ref,
    gate_ref,
    in_ref,
    out_ref,
    into_ref,
    factor_ref,
    skip_ref,
    starts_ref,
    base_ref,
    slope_ref,
    first_ref,
):
    rows, width = stream_ref.shape
    heads = skip_ref.shape[1]
    offset = offset_ref[0]
    starts = starts_ref[...]
    docs = docs_column(starts, offset, rows)
    docs_across = docs_row(starts, offset, rows)
    spread = head_lanes(width, head_size)
    skip = jnp.concatenate(
        [as_column(skip_ref[...], heads), jnp.zeros((PAD - heads, 1), F32)], axis=0
    )
    skip_row = dot_first(two_parts(jnp.broadcast_to(skip, (PAD, LANES))), spread)[:1, :]
    i = lax.broadcasted_iota(jnp.int32, (BLOCK, BLOCK), 0)
    j = lax.broadcasted_iota(jnp.int32, (BLOCK, BLOCK), 1)
    constant_rows = dot_first(into_ref[:, rows:], spread)[:8, :]
    for block in range(rows // BLOCK):
        cut = slice(block * BLOCK, (block + 1) * BLOCK)
        scaled = stream_ref[cut, :].astype(F32) * dot_first(into_ref[:, cut], spread)
        scaled = scaled.astype(BF16)
        if block == 0:
            end = docs[BLOCK - 1 : BLOCK, :]
            to_end = jnp.where(docs[cut, :] == end, in_ref[cut, :].astype(F32), 0.0)
            first_ref[...] = constant_rows[:1, :] * dot_first(to_end.astype(BF16), scaled)
        scores = dot_last(out_ref[cut, :], in_ref[cut, :])
        live = (i >= j) & (docs[cut, :] == docs_across[:, cut])
        weights = jnp.where(live, scores, 0.0).astype(BF16)
        per_lane = dot_first(factor_ref[:, cut], spread)
        within = dot(weights, scaled)
        value = per_lane * within + skip_row * stream_ref[cut, :].astype(F32)
        gate = gate_ref[cut, :].astype(F32)
        gate = gate / (1.0 + jnp.exp(-gate))
        base_ref[cut, :] = value * gate
        slope_ref[cut, :] = per_lane * gate


def link_lanes(links, width, head_size):
    lane = lax.broadcasted_iota(jnp.int32, (LANES, width), 0)
    spot = lax.broadcasted_iota(jnp.int32, (LANES, width), 1)
    head = jnp.where(lane >= PAD, lane - PAD, lane)
    first = head * head_size
    spread = jnp.where(
        (lane < 2 * PAD) & (spot >= first) & (spot < first + head_size), 1.0, 0.0
    ).astype(BF16)
    return dot(links, spread)


def combine_kernel(head_size, core_ref, own_ref, other_ref, pieces_ref):
    states, wide = own_ref.shape
    width = wide - LANES
    half = width // 2
    first_core = core_ref[0] == 0
    own = own_ref[...].astype(F32)
    other = other_ref[...].astype(F32)
    earlier = jnp.where(first_core, own, other)
    later = jnp.where(first_core, other, own)
    rate = link_lanes(later[:8, width:].astype(BF16), width, head_size)[:1, :]
    total = rate * earlier[:, :width] + later[:, :width]
    total = jnp.where(first_core, total[:, :half], total[:, half:])
    parts_a, parts_b = own[:8, width:], other[:8, width:]
    link = (parts_a + pltpu.roll(parts_a, LANES - PAD, 1)) * (
        parts_b + pltpu.roll(parts_b, LANES - PAD, 1)
    )
    lane = lax.broadcasted_iota(jnp.int32, link.shape, 1)
    heads = half // head_size
    link = jnp.where(first_core, link, pltpu.roll(link, LANES - heads, 1))
    link = jnp.where(lane < heads, link, 0.0)
    high = link.astype(BF16).astype(F32)
    link = high + pltpu.roll(link - high, PAD, 1)
    link = jnp.broadcast_to(link[:1, :], (states, LANES))
    pieces_ref[...] = jnp.concatenate([total, link], axis=1).astype(BF16).reshape(pieces_ref.shape)


def scan_kernel(head_size, pieces_ref, before_ref):
    chips, rows, wide = pieces_ref.shape
    width = wide - LANES
    per_lane = link_lanes(pieces_ref[:, 0, width:], width, head_size)
    state = jnp.zeros((rows, width), F32)
    for chip in range(chips):
        before_ref[chip] = state.astype(BF16)
        state = per_lane[chip : chip + 1, :] * state + pieces_ref[chip, :, :width].astype(F32)


def with_squares(piece, squares):
    width = piece.shape[1]
    high = squares.astype(BF16).astype(F32)
    row = jnp.concatenate(
        [high, squares - high, jnp.zeros((1, width - 2 * squares.shape[1]), F32)], axis=1
    )
    return jnp.concatenate(
        [piece.astype(BF16), jnp.broadcast_to(row, (8, width)).astype(BF16)], axis=0
    )


def squares_of(got_ref, step):
    row = got_ref[step:, :].astype(F32)[:1, :]
    return row[:, :step] + row[:, step : 2 * step]


def finish_kernel(
    head_size,
    offset_ref,
    core_ref,
    out_ref,
    before_ref,
    before_other_ref,
    other_ref,
    first_ref,
    factor_ref,
    base_ref,
    slope_ref,
    gain_ref,
    starts_ref,
    hidden_ref,
    squares_ref,
):
    rows, width = base_ref.shape
    offset = offset_ref[0]
    starts = starts_ref[...]
    docs = docs_column(starts, offset, rows)
    before = jnp.max(docs_column(starts, offset - 1, 8)[:1, :], axis=0, keepdims=True)
    spread = head_lanes(width, head_size)
    constant_rows = dot_first(factor_ref[:, rows:], spread)[:8, :]
    first_core = core_ref[0] == 0
    states = other_ref.shape[0]
    half_a = before_ref[...].reshape(states, width // 2).astype(F32)
    half_b = before_other_ref[...].reshape(states, width // 2).astype(F32)
    state = jnp.concatenate(
        [jnp.where(first_core, half_a, half_b), jnp.where(first_core, half_b, half_a)], axis=1
    )
    rate = link_lanes(other_ref[:8, width:], width, head_size)[:1, :]
    state = jnp.where(first_core, state, rate * state + other_ref[:, :width].astype(F32))
    gain = gain_ref[...].reshape(1, width)
    step = rows // 4
    for block in range(rows // BLOCK):
        cut = slice(block * BLOCK, (block + 1) * BLOCK)
        joined = jnp.where(docs[cut, :] == before, out_ref[cut, :].astype(F32), 0.0).astype(BF16)
        carried = dot(joined, (constant_rows[block : block + 1, :] * state).astype(BF16))
        gated = base_ref[cut, :] + slope_ref[cut, :] * carried
        square = gated * gated
        total = square[:, :LANES]
        for lane in range(LANES, width, LANES):
            total = total + square[:, lane : lane + LANES]
        for part in range(BLOCK // step):
            piece = total[part * step : (part + 1) * step, :]
            number = block * (BLOCK // step) + part
            squares_ref[number : number + 1, :] = jnp.sum(
                jnp.transpose(piece), axis=0, keepdims=True
            )
        hidden_ref[cut, :] = (gated * gain).astype(BF16)
        state = constant_rows[2:3, :] * state + first_ref[...]
        before = docs[(block + 1) * BLOCK - 1 : (block + 1) * BLOCK, :]


def far_kernel(y_ref, hidden_ref, proj_ref, squares_ref, send_a_ref, send_b_ref):
    step = hidden_ref.shape[0] // 4
    half = proj_ref.shape[1] // 2
    far = y_ref[0] ^ 2
    piece = hidden_ref[pl.ds(far * step, step), :]
    send_a_ref[...] = with_squares(
        dot(piece, proj_ref[:, :half]), squares_ref[pl.ds(far, 1), :]
    )
    send_b_ref[...] = dot(piece, proj_ref[:, half:]).astype(BF16)


def near_kernel(y_ref, hidden_ref, proj_ref, squares_ref, send_a_ref, send_b_ref):
    step = hidden_ref.shape[0] // 4
    half = proj_ref.shape[1] // 2
    one, three = y_ref[0] ^ 1, y_ref[0] ^ 3
    send_a_ref[...] = with_squares(
        dot(hidden_ref[pl.ds(one * step, step), :], proj_ref[:, :half]),
        squares_ref[pl.ds(one, 1), :],
    )
    send_b_ref[...] = dot(
        hidden_ref[pl.ds(three * step, step), :], proj_ref[:, half:]
    ).astype(BF16)


def keep_kernel(y_ref, hidden_ref, proj_ref, own_ref, via_a_ref, via_b_ref):
    step = hidden_ref.shape[0] // 4
    half = proj_ref.shape[1] // 2
    one, three = y_ref[0] ^ 1, y_ref[0] ^ 3
    via_a_ref[...] = dot(hidden_ref[pl.ds(three * step, step), :], proj_ref[:, :half])
    via_b_ref[...] = dot(hidden_ref[pl.ds(one * step, step), :], proj_ref[:, half:])
    own_ref[...] = dot(hidden_ref[pl.ds(y_ref[0] * step, step), :], proj_ref[...])


def middle_kernel(
    y_ref, squares_ref, via_a_ref, via_b_ref, got_a_ref, got_b_ref, send_a_ref, send_b_ref
):
    step = via_a_ref.shape[0]
    squares = squares_ref[pl.ds(y_ref[0] ^ 3, 1), :] + squares_of(got_a_ref, step)
    send_a_ref[...] = with_squares(via_a_ref[...] + got_a_ref[:step, :].astype(F32), squares)
    send_b_ref[...] = (via_b_ref[...] + got_b_ref[...].astype(F32)).astype(BF16)


def last_kernel(
    channels,
    y_ref,
    squares_ref,
    own_ref,
    near_a_ref,
    near_b_ref,
    far_a_ref,
    far_b_ref,
    out_ref,
):
    step, model = own_ref.shape
    half = model // 2
    squares = squares_ref[pl.ds(y_ref[0], 1), :]
    squares = squares + squares_of(near_a_ref, step) + squares_of(far_a_ref, step)
    scale = as_column(lax.rsqrt(squares / channels + EPSILON), step)
    for near_ref, far_ref, low in ((near_a_ref, far_a_ref, 0), (near_b_ref, far_b_ref, half)):
        total = (
            own_ref[:, low : low + half]
            + near_ref[:step, :].astype(F32)
            + far_ref[:step, :].astype(F32)
        )
        out_ref[:, low : low + half] = (total * scale).astype(BF16)


def call(kernel, out_shape, scalars, arrays, flops, limit, scratch=()):
    single = not isinstance(out_shape, (tuple, list))
    space = HBM_SPEC if scratch else VMEM_SPEC
    return pl.pallas_call(
        kernel,
        out_shape=out_shape,
        in_specs=[SMEM_SPEC] * len(scalars) + [space] * len(arrays),
        out_specs=VMEM_SPEC if single else [VMEM_SPEC] * len(out_shape),
        scratch_shapes=scratch,
        cost_estimate=pl.CostEstimate(flops=flops, bytes_accessed=4_000_000, transcendentals=0),
        compiler_params=pltpu.CompilerParams(vmem_limit_bytes=int(limit * 1024**2)),
    )(*scalars, *arrays)


def local(
    total_channels,
    stream,
    gate_input,
    in_coeff,
    out_coeff,
    step_raw,
    step_bias,
    decay_rate,
    skip_scale,
    norm_gain,
    out_proj,
    doc_starts,
):
    rows, width = stream.shape
    heads = step_raw.shape[0]
    head_size = width // heads
    states = in_coeff.shape[1]
    model = out_proj.shape[1]
    chips = lax.axis_size(CHIPS)
    core = lax.axis_index("seq_2").astype(jnp.int32)[None]
    y = lax.axis_index("head").astype(jnp.int32)[None]
    offset = (lax.axis_index(SEQ) * rows).astype(jnp.int32)[None]
    starts = doc_starts[None, :]
    shape = jax.ShapeDtypeStruct
    arrays = [stream, in_coeff, step_raw, step_bias[None], decay_rate[None], starts]
    summary, into, factor = call(
        functools.partial(state_kernel, head_size),
        [
            shape((states, width + LANES), BF16),
            shape((2 * PAD, rows + LANES), BF16),
            shape((2 * PAD, rows + LANES), BF16),
        ],
        [offset, y, core],
        arrays,
        2_000_000_000,
        FULL,
        [pltpu.VMEM(a.shape, a.dtype) for a in arrays] + [pltpu.SemaphoreType.DMA((len(arrays),))],
    )
    other = lax.ppermute(summary, "seq_2", [(0, 1), (1, 0)])
    pieces = call(
        functools.partial(combine_kernel, head_size),
        shape((chips, states // chips, width // 2 + LANES), BF16),
        [core],
        [summary, other],
        200_000_000,
        8,
    )
    pieces = lax.all_to_all(pieces, CHIPS, 0, 0, tiled=True)
    prior = call(
        functools.partial(scan_kernel, head_size),
        shape((chips, states // chips, width // 2), BF16),
        [],
        [pieces],
        10_000_000_000,
        8,
    )
    incoming = lax.all_to_all(prior, CHIPS, 0, 0, tiled=True)
    incoming_other = lax.ppermute(incoming, "seq_2", [(0, 1), (1, 0)])
    base, slope, first = call(
        functools.partial(within_kernel, head_size),
        [
            shape((rows, width), F32),
            shape((rows, width), F32),
            shape((states, width), F32),
        ],
        [offset],
        [stream, gate_input, in_coeff, out_coeff, into, factor, skip_scale[None], starts],
        4_000_000_000,
        22,
    )
    step = rows // 4
    half = model // 2
    hidden, squares = call(
        functools.partial(finish_kernel, head_size),
        [shape((rows, width), BF16), shape((4, step), F32)],
        [offset, core],
        [out_coeff, incoming, incoming_other, other, first, factor, base, slope, norm_gain, starts],
        1_000_000_000,
        22,
    )
    send_a, send_b = call(
        far_kernel,
        [shape((step + 8, half), BF16), shape((step, half), BF16)],
        [y],
        [hidden, out_proj, squares],
        1_000_000_000,
        16,
    )
    pair_1 = [(i, i ^ 1) for i in range(4)]
    pair_3 = [(i, i ^ 3) for i in range(4)]
    got_a = lax.ppermute(send_a, "head", pair_1)
    got_b = lax.ppermute(send_b, "head", pair_3)
    send_a, send_b = call(
        near_kernel,
        [shape((step + 8, half), BF16), shape((step, half), BF16)],
        [y],
        [hidden, out_proj, squares],
        1_000_000_000,
        16,
    )
    near_a = lax.ppermute(send_a, "head", pair_1)
    near_b = lax.ppermute(send_b, "head", pair_3)
    own, via_a, via_b = call(
        keep_kernel,
        [shape((step, model), F32), shape((step, half), F32), shape((step, half), F32)],
        [y],
        [hidden, out_proj],
        2_000_000_000,
        16,
    )
    send_a, send_b = call(
        middle_kernel,
        [shape((step + 8, half), BF16), shape((step, half), BF16)],
        [y],
        [squares, via_a, via_b, got_a, got_b],
        1_000_000_000,
        8,
    )
    far_a = lax.ppermute(send_a, "head", pair_3)
    far_b = lax.ppermute(send_b, "head", pair_1)
    return call(
        functools.partial(last_kernel, total_channels),
        shape((step, model), BF16),
        [y],
        [squares, own, near_a, near_b, far_a, far_b],
        1_000_000_000,
        8,
    )


def solution(mesh):
    split = Mesh(
        mesh.devices.reshape(4, 8, 2, mesh.shape["head"]), ("seq_0", "seq_1", "seq_2", "head")
    )
    in_specs = (
        P(SEQ, "head"),
        P(SEQ, "head"),
        P(SEQ, None),
        P(SEQ, None),
        P("head", SEQ),
        P("head"),
        P("head"),
        P("head"),
        P("head"),
        P("head", None),
        P(),
    )
    out_specs = P(SEQ_HEAD, None)

    def whole(*args):
        step = functools.partial(local, float(args[0].shape[1]))
        return jax.shard_map(
            step, mesh=split, in_specs=in_specs, out_specs=out_specs, check_vma=False
        )(*args)

    return whole
```

```python
import functools

import jax
import jax.numpy as jnp
from jax import lax
from jax.experimental import pallas as pl
from jax.experimental.pallas import tpu as pltpu
from jax.sharding import Mesh
from jax.sharding import PartitionSpec as P

BLOCK = 256
SEQ = ("seq_0", "seq_1", "seq_2")
CHIPS = ("seq_0", "seq_1")
SEQ_HEAD = ("seq_0", "seq_1", "seq_2", "head")
EPSILON = 1e-05
F32 = jnp.float32
BF16 = jnp.bfloat16
PAD = 32
LANES = 128
FULL = 67_043_328 / 1024**2

VMEM_SPEC = pl.BlockSpec(memory_space=pltpu.VMEM)
SMEM_SPEC = pl.BlockSpec(memory_space=pltpu.SMEM)
HBM_SPEC = pl.BlockSpec(memory_space=pltpu.HBM)


def dot(a, b):
    return jnp.dot(a, b, preferred_element_type=F32)


def dot_first(a, b):
    return lax.dot_general(a, b, (((0,), (0,)), ((), ())), preferred_element_type=F32)


def dot_last(a, b):
    return lax.dot_general(a, b, (((1,), (1,)), ((), ())), preferred_element_type=F32)


def two_parts(value):
    high = value.astype(BF16)
    low = (value - high.astype(F32)).astype(BF16)
    return jnp.concatenate([high, low], axis=0)


def head_lanes(width, head_size):
    row = lax.broadcasted_iota(jnp.int32, (2 * PAD, width), 0)
    lane = lax.broadcasted_iota(jnp.int32, (2 * PAD, width), 1)
    head = jnp.where(row >= PAD, row - PAD, row)
    first = head * head_size
    return jnp.where((lane >= first) & (lane < first + head_size), 1.0, 0.0).astype(BF16)


def as_column(row, count):
    wide = jnp.broadcast_to(row, (count, row.shape[1]))
    i = lax.broadcasted_iota(jnp.int32, wide.shape, 0)
    j = lax.broadcasted_iota(jnp.int32, wide.shape, 1)
    return jnp.sum(jnp.where(i == j, wide, 0.0), axis=1, keepdims=True)


def as_row(column, width):
    wide = jnp.broadcast_to(column, (column.shape[0], width))
    i = lax.broadcasted_iota(jnp.int32, wide.shape, 0)
    j = lax.broadcasted_iota(jnp.int32, wide.shape, 1)
    return jnp.sum(jnp.where(i == j, wide, 0.0), axis=0, keepdims=True)


def docs_column(starts_row, first, count):
    position = first + lax.broadcasted_iota(jnp.int32, (count, starts_row.shape[1]), 0)
    hit = jnp.where(starts_row <= position, 1.0, 0.0)
    return jnp.sum(hit, axis=1, keepdims=True)


def docs_row(starts_row, first, count):
    position = first + lax.broadcasted_iota(jnp.int32, (count, starts_row.shape[1]), 0)
    hit = jnp.where(starts_row <= position, 1.0, 0.0).astype(BF16)
    ones = jnp.ones((8, starts_row.shape[1]), BF16)
    return dot_last(ones, hit)[:1, :]


def state_kernel(
    head_size,
    offset_ref,
    y_ref,
    core_ref,
    stream_hbm,
    in_hbm,
    step_hbm,
    bias_hbm,
    rate_hbm,
    starts_hbm,
    summary_ref,
    first_ref,
    into_ref,
    factor_ref,
    stream_ref,
    in_ref,
    step_ref,
    bias_ref,
    rate_ref,
    starts_ref,
    arrived,
):
    pairs = (
        (step_hbm, step_ref),
        (bias_hbm, bias_ref),
        (rate_hbm, rate_ref),
        (starts_hbm, starts_ref),
        (in_hbm, in_ref),
        (stream_hbm, stream_ref),
    )
    copies = [
        pltpu.make_async_copy(source, target, arrived.at[number])
        for number, (source, target) in enumerate(pairs)
    ]
    for copy in copies:
        copy.start()
    for copy in copies[:4]:
        copy.wait()
    heads, rows = step_ref.shape
    width = stream_ref.shape[1]
    offset = offset_ref[0]
    starts = starts_ref[...]
    docs = docs_column(starts, offset, rows)
    before = jnp.max(docs_column(starts, offset - 1, 8)[:1, :], axis=0, keepdims=True)
    raw = step_ref[...] + as_column(bias_ref[...], heads)
    step = jnp.maximum(raw, 0.0) + jnp.log1p(jnp.exp(-jnp.abs(raw)))
    log_decay = -step * as_column(rate_ref[...], heads)
    i = lax.broadcasted_iota(jnp.int32, (BLOCK, BLOCK), 0)
    j = lax.broadcasted_iota(jnp.int32, (BLOCK, BLOCK), 1)
    upper = jnp.where(i <= j, 1.0, 0.0)
    into, out_of, half, last = [], [], [], []
    for block in range(rows // BLOCK):
        cut = slice(block * BLOCK, (block + 1) * BLOCK)
        cumulative = jnp.dot(
            log_decay[:, cut], upper, precision=lax.Precision.HIGHEST, preferred_element_type=F32
        )
        end = cumulative[:, BLOCK - 1 :]
        middle = 0.5 * end
        into.append(step[:, cut] * jnp.exp(middle - cumulative))
        out_of.append(jnp.exp(cumulative - middle))
        half.append(jnp.exp(middle))
        last.append(end)
    ends = [docs[(b + 1) * BLOCK - 1 : (b + 1) * BLOCK, :] for b in range(rows // BLOCK)]
    joined_0 = jnp.where(ends[0] == before, 1.0, 0.0)
    joined_1 = jnp.where(ends[1] == ends[0], 1.0, 0.0)
    gate_0 = joined_0 * jnp.exp(last[0])
    gate_1 = joined_1 * jnp.exp(last[1])
    link = joined_0 * joined_1 * jnp.exp(last[0] + last[1])
    lane = lax.broadcasted_iota(jnp.int32, (heads, LANES), 1)
    constants = jnp.where(lane == 0, half[0], 0.0)
    constants = jnp.where(lane == 1, half[1], constants)
    constants = jnp.where(lane == 2, gate_0, constants)
    constants = jnp.where(lane == 3, gate_1, constants)
    nothing = jnp.zeros((PAD - heads, rows + LANES), F32)
    spread = head_lanes(width, head_size)
    wide_in = jnp.concatenate([jnp.concatenate(into + [constants], axis=1), nothing], axis=0)
    wide_out = jnp.concatenate([jnp.concatenate(out_of + [constants], axis=1), nothing], axis=0)
    factor_ref[...] = two_parts(wide_out)
    into_parts = two_parts(wide_in)
    into_ref[...] = into_parts
    per_lane = dot_first(into_parts, spread)
    constant_rows = per_lane[rows : rows + 8, :]
    for copy in copies[4:]:
        copy.wait()
    states = []
    for block in range(rows // BLOCK):
        cut = slice(block * BLOCK, (block + 1) * BLOCK)
        scaled = (stream_ref[cut, :].astype(F32) * per_lane[cut, :]).astype(BF16)
        to_end = jnp.where(docs[cut, :] == ends[block], in_ref[cut, :].astype(F32), 0.0)
        states.append(constant_rows[block : block + 1, :] * dot_first(to_end.astype(BF16), scaled))
    first_ref[...] = states[0].astype(BF16)
    summary = constant_rows[3:4, :] * states[0] + states[1]
    high = link.astype(BF16).astype(F32)
    link_row = as_row(high, LANES) + pltpu.roll(as_row(link - high, LANES), PAD, 1)
    whole = jnp.concatenate(
        [summary, jnp.broadcast_to(link_row, (summary.shape[0], LANES))], axis=1
    ).astype(BF16)
    summary_ref[...] = whole


def block_terms(
    head_size,
    offset,
    block,
    stream_ref,
    gate_ref,
    in_ref,
    out_ref,
    into_ref,
    factor_ref,
    skip_ref,
    starts_ref,
):
    rows, width = stream_ref.shape
    heads = skip_ref.shape[1]
    step = rows // 4
    inner = block % (BLOCK // step)
    start = pl.multiple_of(block * step, step)
    origin = pl.multiple_of((block - inner) * step, BLOCK)
    here = pl.ds(start, step)
    whole = pl.ds(origin, BLOCK)
    starts = starts_ref[...]
    docs = docs_column(starts, offset + start, step)
    docs_across = docs_row(starts, offset + origin, BLOCK)
    before = jnp.max(docs_column(starts, offset + origin - 1, 8)[:1, :], axis=0, keepdims=True)
    spread = head_lanes(width, head_size)
    skip = jnp.concatenate(
        [as_column(skip_ref[...], heads), jnp.zeros((PAD - heads, 1), F32)], axis=0
    )
    skip_row = dot_first(two_parts(jnp.broadcast_to(skip, (PAD, LANES))), spread)[:1, :]
    scaled = stream_ref[whole, :].astype(F32) * dot_first(into_ref[:, whole], spread)
    own = out_ref[here, :]
    scores = dot_last(own, in_ref[whole, :])
    i = inner * step + lax.broadcasted_iota(jnp.int32, (step, BLOCK), 0)
    j = lax.broadcasted_iota(jnp.int32, (step, BLOCK), 1)
    live = (i >= j) & (docs == docs_across)
    weights = jnp.where(live, scores, 0.0).astype(BF16)
    per_lane = dot_first(factor_ref[:, here], spread)
    value = per_lane * dot(weights, scaled.astype(BF16)) + skip_row * stream_ref[here, :].astype(F32)
    gate = gate_ref[here, :].astype(F32)
    gate = gate / (1.0 + jnp.exp(-gate))
    joined = jnp.where(docs == before, own.astype(F32), 0.0).astype(BF16)
    return value * gate, per_lane * gate, joined


def block_hidden(base, slope, joined, state, gain):
    gated = base + slope * dot(joined, state)
    square = gated * gated
    total = square[:, :LANES]
    for lane in range(LANES, square.shape[1], LANES):
        total = total + square[:, lane : lane + LANES]
    return (gated * gain).astype(BF16), jnp.sum(jnp.transpose(total), axis=0, keepdims=True)


def ahead_kernel(head_size, offset_ref, y_ref, *refs):
    base_ref, slope_ref, joined_ref = refs[-3:]
    base_ref[...], slope_ref[...], joined_ref[...] = block_terms(
        head_size, offset_ref[0], y_ref[0] ^ 2, *refs[:-3]
    )


def pass_kernel(from_ref, to_ref):
    to_ref[...] = from_ref[...]


def link_lanes(links, width, head_size):
    lane = lax.broadcasted_iota(jnp.int32, (LANES, width), 0)
    spot = lax.broadcasted_iota(jnp.int32, (LANES, width), 1)
    head = jnp.where(lane >= PAD, lane - PAD, lane)
    first = head * head_size
    spread = jnp.where(
        (lane < 2 * PAD) & (spot >= first) & (spot < first + head_size), 1.0, 0.0
    ).astype(BF16)
    return dot(links, spread)


def combine_kernel(head_size, core_ref, own_ref, other_ref, pieces_ref):
    states, wide = own_ref.shape
    width = wide - LANES
    half = width // 2
    first_core = core_ref[0] == 0
    own = own_ref[...].astype(F32)
    other = other_ref[...].astype(F32)
    earlier = jnp.where(first_core, own, other)
    later = jnp.where(first_core, other, own)
    rate = link_lanes(later[:8, width:].astype(BF16), width, head_size)[:1, :]
    total = rate * earlier[:, :width] + later[:, :width]
    total = jnp.where(first_core, total[:, :half], total[:, half:])
    parts_a, parts_b = own[:8, width:], other[:8, width:]
    link = (parts_a + pltpu.roll(parts_a, LANES - PAD, 1)) * (
        parts_b + pltpu.roll(parts_b, LANES - PAD, 1)
    )
    lane = lax.broadcasted_iota(jnp.int32, link.shape, 1)
    heads = half // head_size
    link = jnp.where(first_core, link, pltpu.roll(link, LANES - heads, 1))
    link = jnp.where(lane < heads, link, 0.0)
    high = link.astype(BF16).astype(F32)
    link = high + pltpu.roll(link - high, PAD, 1)
    link = jnp.broadcast_to(link[:1, :], (states, LANES))
    pieces_ref[...] = jnp.concatenate([total, link], axis=1).astype(BF16).reshape(pieces_ref.shape)


def scan_kernel(head_size, pieces_ref, before_ref):
    chips, rows, wide = pieces_ref.shape
    width = wide - LANES
    per_lane = link_lanes(pieces_ref[:, 0, width:], width, head_size)
    state = jnp.zeros((rows, width), F32)
    for chip in range(chips):
        before_ref[chip] = state.astype(BF16)
        state = per_lane[chip : chip + 1, :] * state + pieces_ref[chip, :, :width].astype(F32)


def with_squares(piece, squares):
    width = piece.shape[1]
    high = squares.astype(BF16).astype(F32)
    row = jnp.concatenate(
        [high, squares - high, jnp.zeros((1, width - 2 * squares.shape[1]), F32)], axis=1
    )
    return jnp.concatenate(
        [piece.astype(BF16), jnp.broadcast_to(row, (8, width)).astype(BF16)], axis=0
    )


def squares_of(got_ref, step):
    row = got_ref[step:, :].astype(F32)[:1, :]
    return row[:, :step] + row[:, step : 2 * step]


def state_of(states_ref, block):
    states = states_ref.shape[0] // 2
    return states_ref[pl.ds(pl.multiple_of((block // 2) * states, states), states), :]


def far_kernel(
    head_size,
    y_ref,
    core_ref,
    before_ref,
    before_other_ref,
    other_ref,
    first_ref,
    factor_ref,
    base_ref,
    slope_ref,
    joined_ref,
    gain_ref,
    proj_ref,
    send_a_ref,
    send_b_ref,
    states_ref,
):
    width = base_ref.shape[1]
    states = other_ref.shape[0]
    rows = factor_ref.shape[1] - LANES
    spread = head_lanes(width, head_size)
    constant_rows = dot_first(factor_ref[:, rows:], spread)[:8, :]
    first_core = core_ref[0] == 0
    half_a = before_ref[...].reshape(states, width // 2).astype(F32)
    half_b = before_other_ref[...].reshape(states, width // 2).astype(F32)
    state = jnp.concatenate(
        [jnp.where(first_core, half_a, half_b), jnp.where(first_core, half_b, half_a)], axis=1
    )
    rate = link_lanes(other_ref[:8, width:], width, head_size)[:1, :]
    state = jnp.where(first_core, state, rate * state + other_ref[:, :width].astype(F32))
    states_ref[:states, :] = (constant_rows[:1, :] * state).astype(BF16)
    state = constant_rows[2:3, :] * state + first_ref[...].astype(F32)
    states_ref[states:, :] = (constant_rows[1:2, :] * state).astype(BF16)
    piece, squares = block_hidden(
        base_ref[...],
        slope_ref[...],
        joined_ref[...],
        state_of(states_ref, y_ref[0] ^ 2),
        gain_ref[...].reshape(1, width),
    )
    low = send_b_ref.shape[1]
    send_b_ref[...] = dot(piece, proj_ref[:, -low:]).astype(BF16)
    send_a_ref[...] = with_squares(dot(piece, proj_ref[:, :-low]), squares)


def near_kernel(head_size, offset_ref, y_ref, states_ref, gain_ref, proj_ref, *refs):
    send_a_ref, send_b_ref, hidden_ref, squares_ref = refs[-4:]
    step = refs[0].shape[0] // 4
    low = send_b_ref.shape[1]
    gain = gain_ref[...].reshape(1, -1)
    for number, block in enumerate((y_ref[0] ^ 3, y_ref[0] ^ 1)):
        terms = block_terms(head_size, offset_ref[0], block, *refs[:-4])
        piece, squares = block_hidden(*terms, state_of(states_ref, block), gain)
        hidden_ref[number * step : (number + 1) * step, :] = piece
        if number == 0:
            send_b_ref[...] = dot(piece, proj_ref[:, -low:]).astype(BF16)
            squares_ref[...] = squares
        else:
            send_a_ref[...] = with_squares(dot(piece, proj_ref[:, :-low]), squares)


def keep_kernel(head_size, offset_ref, y_ref, states_ref, gain_ref, proj_ref, hidden_ref, *refs):
    own_ref, via_a_ref, via_b_ref, squares_ref = refs[-4:]
    step = refs[0].shape[0] // 4
    low = via_b_ref.shape[1]
    via_a_ref[...] = dot(hidden_ref[:step, :], proj_ref[:, :-low])
    via_b_ref[...] = dot(hidden_ref[step:, :], proj_ref[:, -low:])
    terms = block_terms(head_size, offset_ref[0], y_ref[0], *refs[:-4])
    piece, squares = block_hidden(
        *terms, state_of(states_ref, y_ref[0]), gain_ref[...].reshape(1, -1)
    )
    squares_ref[...] = squares
    own_ref[...] = dot(piece, proj_ref[...])


def middle_kernel(squares_ref, via_a_ref, via_b_ref, got_a_ref, got_b_ref, send_a_ref, send_b_ref):
    step = via_a_ref.shape[0]
    squares = squares_ref[...] + squares_of(got_a_ref, step)
    send_a_ref[...] = with_squares(via_a_ref[...] + got_a_ref[:step, :].astype(F32), squares)
    send_b_ref[...] = (via_b_ref[...] + got_b_ref[...].astype(F32)).astype(BF16)


def last_kernel(
    channels,
    squares_ref,
    own_ref,
    near_a_ref,
    near_b_ref,
    far_a_ref,
    far_b_ref,
    out_hbm,
    out_ref,
    left,
):
    step, model = own_ref.shape
    edge = near_a_ref.shape[1]
    squares = squares_ref[...]
    squares = squares + squares_of(near_a_ref, step) + squares_of(far_a_ref, step)
    scale = as_column(lax.rsqrt(squares / channels + EPSILON), step)
    chunk = step // 4
    copies = []
    for number in range(4):
        cut = slice(number * chunk, (number + 1) * chunk)
        for near_ref, far_ref, low, high in (
            (near_a_ref, far_a_ref, 0, edge),
            (near_b_ref, far_b_ref, edge, model),
        ):
            total = (
                own_ref[cut, low:high]
                + near_ref[cut, :].astype(F32)
                + far_ref[cut, :].astype(F32)
            )
            out_ref[cut, low:high] = (total * scale[cut, :]).astype(BF16)
        here = pl.ds(number * chunk, chunk)
        copy = pltpu.make_async_copy(out_ref.at[here, :], out_hbm.at[here, :], left.at[number])
        copy.start()
        copies.append(copy)
    for copy in copies:
        copy.wait()


def call(kernel, out_shape, scalars, arrays, flops, limit, scratch=(), space=VMEM_SPEC, result=VMEM_SPEC):
    single = not isinstance(out_shape, (tuple, list))
    return pl.pallas_call(
        kernel,
        out_shape=out_shape,
        in_specs=[SMEM_SPEC] * len(scalars) + [space] * len(arrays),
        out_specs=result if single else [result] * len(out_shape),
        scratch_shapes=scratch,
        cost_estimate=pl.CostEstimate(flops=flops, bytes_accessed=4_000_000, transcendentals=0),
        compiler_params=pltpu.CompilerParams(vmem_limit_bytes=int(limit * 1024**2)),
    )(*scalars, *arrays)


def local(
    total_channels,
    stream,
    gate_input,
    in_coeff,
    out_coeff,
    step_raw,
    step_bias,
    decay_rate,
    skip_scale,
    norm_gain,
    out_proj,
    doc_starts,
):
    rows, width = stream.shape
    heads = step_raw.shape[0]
    head_size = width // heads
    states = in_coeff.shape[1]
    model = out_proj.shape[1]
    chips = lax.axis_size(CHIPS)
    core = lax.axis_index("seq_2").astype(jnp.int32)[None]
    y = lax.axis_index("head").astype(jnp.int32)[None]
    offset = (lax.axis_index(SEQ) * rows).astype(jnp.int32)[None]
    starts = doc_starts[None, :]
    shape = jax.ShapeDtypeStruct
    arrays = [stream, in_coeff, step_raw, step_bias[None], decay_rate[None], starts]
    summary, first, into, factor = call(
        functools.partial(state_kernel, head_size),
        [
            shape((states, width + LANES), BF16),
            shape((states, width), BF16),
            shape((2 * PAD, rows + LANES), BF16),
            shape((2 * PAD, rows + LANES), BF16),
        ],
        [offset, y, core],
        arrays,
        2_000_000_000,
        FULL,
        [pltpu.VMEM(a.shape, a.dtype) for a in arrays] + [pltpu.SemaphoreType.DMA((len(arrays),))],
        HBM_SPEC,
    )
    other = lax.ppermute(summary, "seq_2", [(0, 1), (1, 0)])
    own = call(pass_kernel, shape(summary.shape, BF16), [], [summary], 100_000_000, 4)
    pieces = call(
        functools.partial(combine_kernel, head_size),
        shape((chips, states // chips, width // 2 + LANES), BF16),
        [core],
        [own, other],
        200_000_000,
        8,
    )
    pieces = lax.all_to_all(pieces, CHIPS, 0, 0, tiled=True)
    prior = call(
        functools.partial(scan_kernel, head_size),
        shape((chips, states // chips, width // 2), BF16),
        [],
        [pieces],
        10_000_000_000,
        8,
    )
    incoming = lax.all_to_all(prior, CHIPS, 0, 0, tiled=True)
    incoming_other = lax.ppermute(incoming, "seq_2", [(0, 1), (1, 0)])
    step = rows // 4
    edge = model * 11 // 20
    rest = model - edge
    tokens = [
        stream,
        gate_input,
        in_coeff,
        out_coeff,
        into,
        factor,
        skip_scale[None],
        starts,
    ]
    base, slope, joined = call(
        functools.partial(ahead_kernel, head_size),
        [shape((step, width), F32), shape((step, width), F32), shape((step, states), BF16)],
        [offset, y],
        tokens,
        2_000_000_000,
        16,
    )
    send_a, send_b, ready = call(
        functools.partial(far_kernel, head_size),
        [
            shape((step + 8, edge), BF16),
            shape((step, rest), BF16),
            shape((2 * states, width), BF16),
        ],
        [y, core],
        [
            incoming,
            incoming_other,
            other,
            first,
            factor,
            base,
            slope,
            joined,
            norm_gain,
            out_proj,
        ],
        1_000_000_000,
        16,
    )
    pair_1 = [(i, i ^ 1) for i in range(4)]
    pair_3 = [(i, i ^ 3) for i in range(4)]
    got_a = lax.ppermute(send_a, "head", pair_1)
    got_b = lax.ppermute(send_b, "head", pair_3)
    send_a, send_b, hidden, via_squares = call(
        functools.partial(near_kernel, head_size),
        [
            shape((step + 8, edge), BF16),
            shape((step, rest), BF16),
            shape((2 * step, width), BF16),
            shape((1, step), F32),
        ],
        [offset, y],
        [ready, norm_gain, out_proj] + tokens,
        2_000_000_000,
        20,
    )
    near_a = lax.ppermute(send_a, "head", pair_1)
    near_b = lax.ppermute(send_b, "head", pair_3)
    own, via_a, via_b, squares = call(
        functools.partial(keep_kernel, head_size),
        [
            shape((step, model), F32),
            shape((step, edge), F32),
            shape((step, rest), F32),
            shape((1, step), F32),
        ],
        [offset, y],
        [ready, norm_gain, out_proj, hidden] + tokens,
        2_000_000_000,
        20,
    )
    send_a, send_b = call(
        middle_kernel,
        [shape((step + 8, edge), BF16), shape((step, rest), BF16)],
        [],
        [via_squares, via_a, via_b, got_a, got_b],
        1_000_000_000,
        8,
    )
    far_a = lax.ppermute(send_a, "head", pair_3)
    far_b = lax.ppermute(send_b, "head", pair_1)
    return call(
        functools.partial(last_kernel, total_channels),
        shape((step, model), BF16),
        [],
        [squares, own, near_a, near_b, far_a, far_b],
        1_000_000_000,
        8,
        [pltpu.VMEM((step, model), BF16), pltpu.SemaphoreType.DMA((4,))],
        VMEM_SPEC,
        HBM_SPEC,
    )


def solution(mesh):
    split = Mesh(
        mesh.devices.reshape(4, 8, 2, mesh.shape["head"]), ("seq_0", "seq_1", "seq_2", "head")
    )
    in_specs = (
        P(SEQ, "head"),
        P(SEQ, "head"),
        P(SEQ, None),
        P(SEQ, None),
        P("head", SEQ),
        P("head"),
        P("head"),
        P("head"),
        P("head"),
        P("head", None),
        P(),
    )
    out_specs = P(SEQ_HEAD, None)

    def whole(*args):
        step = functools.partial(local, float(args[0].shape[1]))
        return jax.shard_map(
            step, mesh=split, in_specs=in_specs, out_specs=out_specs, check_vma=False
        )(*args)

    return whole
```

```python
import functools

import jax
import jax.numpy as jnp
from jax import lax
from jax.experimental import pallas as pl
from jax.experimental.pallas import tpu as pltpu
from jax.sharding import Mesh
from jax.sharding import PartitionSpec as P

BLOCK = 256
SEQ = ("seq_0", "seq_1", "seq_2")
CHIPS = ("seq_0", "seq_1")
SEQ_HEAD = ("seq_0", "seq_1", "seq_2", "head")
EPSILON = 1e-05
F32 = jnp.float32
BF16 = jnp.bfloat16
PAD = 32
LANES = 128

VMEM_SPEC = pl.BlockSpec(memory_space=pltpu.VMEM)
SMEM_SPEC = pl.BlockSpec(memory_space=pltpu.SMEM)
HBM_SPEC = pl.BlockSpec(memory_space=pltpu.HBM)


def dot(a, b):
    return jnp.dot(a, b, preferred_element_type=F32)


def dot_first(a, b):
    return lax.dot_general(a, b, (((0,), (0,)), ((), ())), preferred_element_type=F32)


def dot_last(a, b):
    return lax.dot_general(a, b, (((1,), (1,)), ((), ())), preferred_element_type=F32)


def two_parts(value):
    high = value.astype(BF16)
    low = (value - high.astype(F32)).astype(BF16)
    return jnp.concatenate([high, low], axis=0)


def head_lanes(width, head_size):
    row = lax.broadcasted_iota(jnp.int32, (2 * PAD, width), 0)
    lane = lax.broadcasted_iota(jnp.int32, (2 * PAD, width), 1)
    head = jnp.where(row >= PAD, row - PAD, row)
    first = head * head_size
    return jnp.where((lane >= first) & (lane < first + head_size), 1.0, 0.0).astype(BF16)


def as_column(row, count):
    wide = jnp.broadcast_to(row, (count, row.shape[1]))
    i = lax.broadcasted_iota(jnp.int32, wide.shape, 0)
    j = lax.broadcasted_iota(jnp.int32, wide.shape, 1)
    return jnp.sum(jnp.where(i == j, wide, 0.0), axis=1, keepdims=True)


def as_row(column, width):
    wide = jnp.broadcast_to(column, (column.shape[0], width))
    i = lax.broadcasted_iota(jnp.int32, wide.shape, 0)
    j = lax.broadcasted_iota(jnp.int32, wide.shape, 1)
    return jnp.sum(jnp.where(i == j, wide, 0.0), axis=0, keepdims=True)


def docs_column(starts_row, first, count):
    position = first + lax.broadcasted_iota(jnp.int32, (count, starts_row.shape[1]), 0)
    hit = jnp.where(starts_row <= position, 1.0, 0.0)
    return jnp.sum(hit, axis=1, keepdims=True)


def docs_row(starts_row, first, count):
    position = first + lax.broadcasted_iota(jnp.int32, (count, starts_row.shape[1]), 0)
    hit = jnp.where(starts_row <= position, 1.0, 0.0).astype(BF16)
    ones = jnp.ones((8, starts_row.shape[1]), BF16)
    return dot_last(ones, hit)[:1, :]


def state_kernel(
    head_size,
    offset_ref,
    y_ref,
    core_ref,
    stream_hbm,
    in_hbm,
    step_hbm,
    bias_hbm,
    rate_hbm,
    starts_hbm,
    summary_ref,
    first_ref,
    into_ref,
    factor_ref,
    stream_ref,
    in_ref,
    step_ref,
    bias_ref,
    rate_ref,
    starts_ref,
    arrived,
):
    pairs = (
        (step_hbm, step_ref),
        (bias_hbm, bias_ref),
        (rate_hbm, rate_ref),
        (starts_hbm, starts_ref),
        (in_hbm, in_ref),
        (stream_hbm, stream_ref),
    )
    copies = [
        pltpu.make_async_copy(source, target, arrived.at[number])
        for number, (source, target) in enumerate(pairs)
    ]
    for copy in copies:
        copy.start()
    heads, rows = step_ref.shape
    width = stream_ref.shape[1]
    spread = head_lanes(width, head_size)
    i = lax.broadcasted_iota(jnp.int32, (BLOCK, BLOCK), 0)
    j = lax.broadcasted_iota(jnp.int32, (BLOCK, BLOCK), 1)
    upper = jnp.where(i <= j, 1.0, 0.0)
    for copy in copies[:4]:
        copy.wait()
    offset = offset_ref[0]
    starts = starts_ref[...]
    docs = docs_column(starts, offset, rows)
    before = jnp.max(docs_column(starts, offset - 1, 8)[:1, :], axis=0, keepdims=True)
    raw = step_ref[...] + as_column(bias_ref[...], heads)
    step = jnp.maximum(raw, 0.0) + jnp.log1p(jnp.exp(-jnp.abs(raw)))
    log_decay = -step * as_column(rate_ref[...], heads)
    into, out_of, half, last = [], [], [], []
    for block in range(rows // BLOCK):
        cut = slice(block * BLOCK, (block + 1) * BLOCK)
        cumulative = jnp.dot(
            log_decay[:, cut], upper, precision=lax.Precision.HIGHEST, preferred_element_type=F32
        )
        end = cumulative[:, BLOCK - 1 :]
        middle = 0.5 * end
        into.append(step[:, cut] * jnp.exp(middle - cumulative))
        out_of.append(jnp.exp(cumulative - middle))
        half.append(jnp.exp(middle))
        last.append(end)
    ends = [docs[(b + 1) * BLOCK - 1 : (b + 1) * BLOCK, :] for b in range(rows // BLOCK)]
    joined_0 = jnp.where(ends[0] == before, 1.0, 0.0)
    joined_1 = jnp.where(ends[1] == ends[0], 1.0, 0.0)
    gate_0 = joined_0 * jnp.exp(last[0])
    gate_1 = joined_1 * jnp.exp(last[1])
    link = joined_0 * joined_1 * jnp.exp(last[0] + last[1])
    lane = lax.broadcasted_iota(jnp.int32, (heads, LANES), 1)
    constants = jnp.where(lane == 0, half[0], 0.0)
    constants = jnp.where(lane == 1, half[1], constants)
    constants = jnp.where(lane == 2, gate_0, constants)
    constants = jnp.where(lane == 3, gate_1, constants)
    nothing = jnp.zeros((PAD - heads, rows + LANES), F32)
    wide_in = jnp.concatenate([jnp.concatenate(into + [constants], axis=1), nothing], axis=0)
    wide_out = jnp.concatenate([jnp.concatenate(out_of + [constants], axis=1), nothing], axis=0)
    factor_ref[...] = two_parts(wide_out)
    into_parts = two_parts(wide_in)
    into_ref[...] = into_parts
    per_lane = dot_first(into_parts, spread)
    constant_rows = per_lane[rows : rows + 8, :]
    for copy in copies[4:]:
        copy.wait()
    states = []
    for block in range(rows // BLOCK):
        cut = slice(block * BLOCK, (block + 1) * BLOCK)
        scaled = (stream_ref[cut, :].astype(F32) * per_lane[cut, :]).astype(BF16)
        to_end = jnp.where(docs[cut, :] == ends[block], in_ref[cut, :].astype(F32), 0.0)
        states.append(constant_rows[block : block + 1, :] * dot_first(to_end.astype(BF16), scaled))
    first_ref[...] = states[0].astype(BF16)
    summary = constant_rows[3:4, :] * states[0] + states[1]
    high = link.astype(BF16).astype(F32)
    link_row = as_row(high, LANES) + pltpu.roll(as_row(link - high, LANES), PAD, 1)
    whole = jnp.concatenate(
        [summary, jnp.broadcast_to(link_row, (summary.shape[0], LANES))], axis=1
    ).astype(BF16)
    summary_ref[...] = whole


def block_terms(
    head_size,
    offset,
    block,
    stream_ref,
    gate_ref,
    in_ref,
    out_ref,
    into_ref,
    factor_ref,
    skip_ref,
    starts_ref,
):
    rows, width = stream_ref.shape
    heads = skip_ref.shape[1]
    step = rows // 4
    inner = block % (BLOCK // step)
    start = pl.multiple_of(block * step, step)
    origin = pl.multiple_of((block - inner) * step, BLOCK)
    here = pl.ds(start, step)
    whole = pl.ds(origin, BLOCK)
    starts = starts_ref[...]
    docs = docs_column(starts, offset + start, step)
    docs_across = docs_row(starts, offset + origin, BLOCK)
    before = jnp.max(docs_column(starts, offset + origin - 1, 8)[:1, :], axis=0, keepdims=True)
    spread = head_lanes(width, head_size)
    skip = jnp.concatenate(
        [as_column(skip_ref[...], heads), jnp.zeros((PAD - heads, 1), F32)], axis=0
    )
    skip_row = dot_first(two_parts(jnp.broadcast_to(skip, (PAD, LANES))), spread)[:1, :]
    scaled = stream_ref[whole, :].astype(F32) * dot_first(into_ref[:, whole], spread)
    own = out_ref[here, :]
    scores = dot_last(own, in_ref[whole, :])
    i = inner * step + lax.broadcasted_iota(jnp.int32, (step, BLOCK), 0)
    j = lax.broadcasted_iota(jnp.int32, (step, BLOCK), 1)
    live = (i >= j) & (docs == docs_across)
    weights = jnp.where(live, scores, 0.0).astype(BF16)
    per_lane = dot_first(factor_ref[:, here], spread)
    value = per_lane * dot(weights, scaled.astype(BF16)) + skip_row * stream_ref[here, :].astype(F32)
    gate = gate_ref[here, :].astype(F32)
    gate = gate / (1.0 + jnp.exp(-gate))
    joined = jnp.where(docs == before, own.astype(F32), 0.0).astype(BF16)
    return value * gate, per_lane * gate, joined


def block_hidden(base, slope, joined, state, gain):
    gated = base + slope * dot(joined, state)
    square = gated * gated
    total = square[:, :LANES]
    for lane in range(LANES, square.shape[1], LANES):
        total = total + square[:, lane : lane + LANES]
    return (gated * gain).astype(BF16), jnp.sum(jnp.transpose(total), axis=0, keepdims=True)


def ahead_kernel(head_size, offset_ref, y_ref, other_ref, *refs):
    base_ref, slope_ref, joined_ref, lanes_ref = refs[-4:]
    base_ref[...], slope_ref[...], joined_ref[...] = block_terms(
        head_size, offset_ref[0], y_ref[0] ^ 2, *refs[:-4]
    )
    rows, width = refs[0].shape
    factor_ref = refs[5]
    lanes_ref[:8, :] = dot_first(factor_ref[:, rows:], head_lanes(width, head_size))[:8, :]
    lanes_ref[8:, :] = link_lanes(other_ref[:8, width:], width, head_size)


def link_lanes(links, width, head_size):
    lane = lax.broadcasted_iota(jnp.int32, (LANES, width), 0)
    spot = lax.broadcasted_iota(jnp.int32, (LANES, width), 1)
    head = jnp.where(lane >= PAD, lane - PAD, lane)
    first = head * head_size
    spread = jnp.where(
        (lane < 2 * PAD) & (spot >= first) & (spot < first + head_size), 1.0, 0.0
    ).astype(BF16)
    return dot(links, spread)


def combine_kernel(head_size, core_ref, own_ref, other_ref, pieces_ref):
    states, wide = own_ref.shape
    width = wide - LANES
    half = width // 2
    first_core = core_ref[0] == 0
    own = own_ref[...].astype(F32)
    other = other_ref[...].astype(F32)
    earlier = jnp.where(first_core, own, other)
    later = jnp.where(first_core, other, own)
    rate = link_lanes(later[:8, width:].astype(BF16), width, head_size)[:1, :]
    total = rate * earlier[:, :width] + later[:, :width]
    total = jnp.where(first_core, total[:, :half], total[:, half:])
    parts_a, parts_b = own[:8, width:], other[:8, width:]
    link = (parts_a + pltpu.roll(parts_a, LANES - PAD, 1)) * (
        parts_b + pltpu.roll(parts_b, LANES - PAD, 1)
    )
    lane = lax.broadcasted_iota(jnp.int32, link.shape, 1)
    heads = half // head_size
    link = jnp.where(first_core, link, pltpu.roll(link, LANES - heads, 1))
    link = jnp.where(lane < heads, link, 0.0)
    high = link.astype(BF16).astype(F32)
    link = high + pltpu.roll(link - high, PAD, 1)
    link = jnp.broadcast_to(link[:1, :], (states, LANES))
    pieces_ref[...] = jnp.concatenate([total, link], axis=1).astype(BF16).reshape(pieces_ref.shape)


def scan_kernel(head_size, pieces_ref, before_ref):
    chips, rows, wide = pieces_ref.shape
    width = wide - LANES
    per_lane = link_lanes(pieces_ref[:, 0, width:], width, head_size)
    state = jnp.zeros((rows, width), F32)
    for chip in range(chips):
        before_ref[chip] = state.astype(BF16)
        state = per_lane[chip : chip + 1, :] * state + pieces_ref[chip, :, :width].astype(F32)


def with_squares(piece, squares):
    width = piece.shape[1]
    high = squares.astype(BF16).astype(F32)
    row = jnp.concatenate(
        [high, squares - high, jnp.zeros((1, width - 2 * squares.shape[1]), F32)], axis=1
    )
    return jnp.concatenate(
        [piece.astype(BF16), jnp.broadcast_to(row, (8, width)).astype(BF16)], axis=0
    )


def squares_of(got_ref, step):
    row = got_ref[step:, :].astype(F32)[:1, :]
    return row[:, :step] + row[:, step : 2 * step]


def state_of(states_ref, block):
    states = states_ref.shape[0] // 2
    return states_ref[pl.ds(pl.multiple_of((block // 2) * states, states), states), :]


def far_kernel(
    y_ref,
    core_ref,
    before_ref,
    before_other_ref,
    other_ref,
    first_ref,
    lanes_ref,
    base_ref,
    slope_ref,
    joined_ref,
    gain_ref,
    proj_ref,
    send_a_ref,
    hidden_ref,
    states_ref,
    squares_ref,
):
    width = base_ref.shape[1]
    states = other_ref.shape[0]
    constant_rows = lanes_ref[:8, :]
    first_core = core_ref[0] == 0
    half_a = before_ref[...].reshape(states, width // 2).astype(F32)
    half_b = before_other_ref[...].reshape(states, width // 2).astype(F32)
    state = jnp.concatenate(
        [jnp.where(first_core, half_a, half_b), jnp.where(first_core, half_b, half_a)], axis=1
    )
    rate = lanes_ref[8:9, :]
    state = jnp.where(first_core, state, rate * state + other_ref[:, :width].astype(F32))
    states_ref[:states, :] = (constant_rows[:1, :] * state).astype(BF16)
    state = constant_rows[2:3, :] * state + first_ref[...].astype(F32)
    states_ref[states:, :] = (constant_rows[1:2, :] * state).astype(BF16)
    piece, squares = block_hidden(
        base_ref[...],
        slope_ref[...],
        joined_ref[...],
        state_of(states_ref, y_ref[0] ^ 2),
        gain_ref[...].reshape(1, width),
    )
    hidden_ref[...] = piece
    squares_ref[...] = squares
    send_a_ref[...] = dot(piece, proj_ref[:, : send_a_ref.shape[1]]).astype(BF16)


def far_b_kernel(hidden_ref, proj_ref, squares_ref, send_b_ref):
    send_b_ref[...] = with_squares(
        dot(hidden_ref[...], proj_ref[:, -send_b_ref.shape[1] :]), squares_ref[...]
    )


def near_kernel(head_size, offset_ref, y_ref, states_ref, gain_ref, proj_ref, *refs):
    send_a_ref, send_b_ref, hidden_ref, squares_ref = refs[-4:]
    step = refs[0].shape[0] // 4
    low = send_b_ref.shape[1]
    gain = gain_ref[...].reshape(1, -1)
    for number, block in enumerate((y_ref[0] ^ 3, y_ref[0] ^ 1)):
        terms = block_terms(head_size, offset_ref[0], block, *refs[:-4])
        piece, squares = block_hidden(*terms, state_of(states_ref, block), gain)
        hidden_ref[number * step : (number + 1) * step, :] = piece
        if number == 0:
            send_b_ref[...] = with_squares(dot(piece, proj_ref[:, -low:]), squares)
        else:
            send_a_ref[...] = dot(piece, proj_ref[:, :-low]).astype(BF16)
            squares_ref[...] = squares


def keep_kernel(head_size, offset_ref, y_ref, states_ref, gain_ref, proj_ref, hidden_ref, *refs):
    own_ref, via_a_ref, via_b_ref, squares_ref = refs[-4:]
    step = refs[0].shape[0] // 4
    low = via_b_ref.shape[1]
    via_a_ref[...] = dot(hidden_ref[:step, :], proj_ref[:, :-low])
    via_b_ref[...] = dot(hidden_ref[step:, :], proj_ref[:, -low:])
    terms = block_terms(head_size, offset_ref[0], y_ref[0], *refs[:-4])
    piece, squares = block_hidden(
        *terms, state_of(states_ref, y_ref[0]), gain_ref[...].reshape(1, -1)
    )
    squares_ref[...] = squares
    own_ref[...] = dot(piece, proj_ref[...])


def middle_kernel(squares_ref, via_a_ref, via_b_ref, got_a_ref, got_b_ref, send_a_ref, send_b_ref):
    step = via_a_ref.shape[0]
    squares = squares_ref[...] + squares_of(got_b_ref, step)
    send_a_ref[...] = (via_a_ref[...] + got_a_ref[...].astype(F32)).astype(BF16)
    send_b_ref[...] = with_squares(via_b_ref[...] + got_b_ref[:step, :].astype(F32), squares)


def last_kernel(
    channels,
    squares_ref,
    own_ref,
    near_a_ref,
    near_b_ref,
    far_a_ref,
    far_b_ref,
    out_hbm,
    out_ref,
    left,
):
    step, model = own_ref.shape
    edge = near_a_ref.shape[1]
    squares = squares_ref[...]
    squares = squares + squares_of(near_b_ref, step) + squares_of(far_b_ref, step)
    scale = as_column(lax.rsqrt(squares / channels + EPSILON), step)
    chunk = step // 4
    copies = []
    for number in range(4):
        cut = slice(number * chunk, (number + 1) * chunk)
        for near_ref, far_ref, low, high in (
            (near_a_ref, far_a_ref, 0, edge),
            (near_b_ref, far_b_ref, edge, model),
        ):
            total = (
                own_ref[cut, low:high]
                + near_ref[cut, :].astype(F32)
                + far_ref[cut, :].astype(F32)
            )
            out_ref[cut, low:high] = (total * scale[cut, :]).astype(BF16)
        here = pl.ds(number * chunk, chunk)
        copy = pltpu.make_async_copy(out_ref.at[here, :], out_hbm.at[here, :], left.at[number])
        copy.start()
        copies.append(copy)
    for copy in copies:
        copy.wait()


def call(kernel, out_shape, scalars, arrays, flops, limit, scratch=(), space=VMEM_SPEC, result=VMEM_SPEC):
    single = not isinstance(out_shape, (tuple, list))
    return pl.pallas_call(
        kernel,
        out_shape=out_shape,
        in_specs=[SMEM_SPEC] * len(scalars) + [space] * len(arrays),
        out_specs=result if single else [result] * len(out_shape),
        scratch_shapes=scratch,
        cost_estimate=pl.CostEstimate(flops=flops, bytes_accessed=4_000_000, transcendentals=0),
        compiler_params=pltpu.CompilerParams(vmem_limit_bytes=int(limit * 1024**2)),
    )(*scalars, *arrays)


def local(
    total_channels,
    stream,
    gate_input,
    in_coeff,
    out_coeff,
    step_raw,
    step_bias,
    decay_rate,
    skip_scale,
    norm_gain,
    out_proj,
    doc_starts,
):
    rows, width = stream.shape
    heads = step_raw.shape[0]
    head_size = width // heads
    states = in_coeff.shape[1]
    model = out_proj.shape[1]
    chips = lax.axis_size(CHIPS)
    core = lax.axis_index("seq_2").astype(jnp.int32)[None]
    y = lax.axis_index("head").astype(jnp.int32)[None]
    offset = (lax.axis_index(SEQ) * rows).astype(jnp.int32)[None]
    starts = doc_starts[None, :]
    shape = jax.ShapeDtypeStruct
    arrays = [
        pltpu.with_memory_space_constraint(a, pltpu.HBM)
        for a in (stream, in_coeff, step_raw, step_bias[None], decay_rate[None], starts)
    ]
    summary, first, into, factor = call(
        functools.partial(state_kernel, head_size),
        [
            shape((states, width + LANES), BF16),
            shape((states, width), BF16),
            shape((2 * PAD, rows + LANES), BF16),
            shape((2 * PAD, rows + LANES), BF16),
        ],
        [offset, y, core],
        arrays,
        2_000_000_000,
        24,
        [pltpu.VMEM(a.shape, a.dtype) for a in arrays] + [pltpu.SemaphoreType.DMA((len(arrays),))],
        HBM_SPEC,
    )
    other = lax.ppermute(summary, "seq_2", [(0, 1), (1, 0)])
    pieces = call(
        functools.partial(combine_kernel, head_size),
        shape((chips, states // chips, width // 2 + LANES), BF16),
        [core],
        [summary, other],
        200_000_000,
        8,
    )
    pieces = lax.all_to_all(pieces, CHIPS, 0, 0, tiled=True)
    prior = call(
        functools.partial(scan_kernel, head_size),
        shape((chips, states // chips, width // 2), BF16),
        [],
        [pieces],
        10_000_000_000,
        8,
    )
    incoming = lax.all_to_all(prior, CHIPS, 0, 0, tiled=True)
    incoming_other = lax.ppermute(incoming, "seq_2", [(0, 1), (1, 0)])
    step = rows // 4
    edge = model * 12 // 20
    rest = model - edge
    tokens = [
        stream,
        gate_input,
        in_coeff,
        out_coeff,
        into,
        factor,
        skip_scale[None],
        starts,
    ]
    base, slope, joined, lanes = call(
        functools.partial(ahead_kernel, head_size),
        [
            shape((step, width), F32),
            shape((step, width), F32),
            shape((step, states), BF16),
            shape((16, width), F32),
        ],
        [offset, y],
        [other] + tokens,
        2_000_000_000,
        16,
    )
    send_a, hidden, ready, squares = call(
        far_kernel,
        [
            shape((step, edge), BF16),
            shape((step, width), BF16),
            shape((2 * states, width), BF16),
            shape((1, step), F32),
        ],
        [y, core],
        [
            incoming,
            incoming_other,
            other,
            first,
            lanes,
            base,
            slope,
            joined,
            norm_gain,
            out_proj,
        ],
        1_000_000_000,
        16,
    )
    pair_1 = [(i, i ^ 1) for i in range(4)]
    pair_3 = [(i, i ^ 3) for i in range(4)]
    got_a = lax.ppermute(send_a, "head", pair_1)
    send_b = call(
        far_b_kernel,
        shape((step + 8, rest), BF16),
        [],
        [hidden, out_proj, squares],
        400_000_000,
        12,
    )
    got_b = lax.ppermute(send_b, "head", pair_3)
    send_a, send_b, hidden, via_squares = call(
        functools.partial(near_kernel, head_size),
        [
            shape((step, edge), BF16),
            shape((step + 8, rest), BF16),
            shape((2 * step, width), BF16),
            shape((1, step), F32),
        ],
        [offset, y],
        [ready, norm_gain, out_proj] + tokens,
        2_000_000_000,
        20,
    )
    near_a = lax.ppermute(send_a, "head", pair_1)
    near_b = lax.ppermute(send_b, "head", pair_3)
    own, via_a, via_b, squares = call(
        functools.partial(keep_kernel, head_size),
        [
            shape((step, model), F32),
            shape((step, edge), F32),
            shape((step, rest), F32),
            shape((1, step), F32),
        ],
        [offset, y],
        [ready, norm_gain, out_proj, hidden] + tokens,
        2_000_000_000,
        20,
    )
    send_a, send_b = call(
        middle_kernel,
        [shape((step, edge), BF16), shape((step + 8, rest), BF16)],
        [],
        [via_squares, via_a, via_b, got_a, got_b],
        1_000_000_000,
        8,
    )
    far_a = lax.ppermute(send_a, "head", pair_3)
    far_b = lax.ppermute(send_b, "head", pair_1)
    return call(
        functools.partial(last_kernel, total_channels),
        shape((step, model), BF16),
        [],
        [squares, own, near_a, near_b, far_a, far_b],
        1_000_000_000,
        8,
        [pltpu.VMEM((step, model), BF16), pltpu.SemaphoreType.DMA((4,))],
        VMEM_SPEC,
        HBM_SPEC,
    )


def solution(mesh):
    split = Mesh(
        mesh.devices.reshape(4, 8, 2, mesh.shape["head"]), ("seq_0", "seq_1", "seq_2", "head")
    )
    in_specs = (
        P(SEQ, "head"),
        P(SEQ, "head"),
        P(SEQ, None),
        P(SEQ, None),
        P("head", SEQ),
        P("head"),
        P("head"),
        P("head"),
        P("head"),
        P("head", None),
        P(),
    )
    out_specs = P(SEQ_HEAD, None)

    def whole(*args):
        step = functools.partial(local, float(args[0].shape[1]))
        return jax.shard_map(
            step, mesh=split, in_specs=in_specs, out_specs=out_specs, check_vma=False
        )(*args)

    return whole
```

```python
import functools

import jax
import jax.numpy as jnp
from jax import lax
from jax.experimental import pallas as pl
from jax.experimental.pallas import tpu as pltpu
from jax.sharding import Mesh
from jax.sharding import PartitionSpec as P

BLOCK = 256
SEQ = ("seq_0", "seq_1", "seq_2")
CHIPS = ("seq_0", "seq_1")
SEQ_HEAD = ("seq_0", "seq_1", "seq_2", "head")
EPSILON = 1e-05
F32 = jnp.float32
BF16 = jnp.bfloat16
PAD = 32
LANES = 128

VMEM_SPEC = pl.BlockSpec(memory_space=pltpu.VMEM)
SMEM_SPEC = pl.BlockSpec(memory_space=pltpu.SMEM)
HBM_SPEC = pl.BlockSpec(memory_space=pltpu.HBM)


def dot(a, b):
    return jnp.dot(a, b, preferred_element_type=F32)


def dot_first(a, b):
    return lax.dot_general(a, b, (((0,), (0,)), ((), ())), preferred_element_type=F32)


def dot_last(a, b):
    return lax.dot_general(a, b, (((1,), (1,)), ((), ())), preferred_element_type=F32)


def two_parts(value):
    high = value.astype(BF16)
    low = (value - high.astype(F32)).astype(BF16)
    return jnp.concatenate([high, low], axis=0)


def head_lanes(width, head_size):
    row = lax.broadcasted_iota(jnp.int32, (2 * PAD, width), 0)
    lane = lax.broadcasted_iota(jnp.int32, (2 * PAD, width), 1)
    head = jnp.where(row >= PAD, row - PAD, row)
    first = head * head_size
    return jnp.where((lane >= first) & (lane < first + head_size), 1.0, 0.0).astype(BF16)


def as_column(row, count):
    wide = jnp.broadcast_to(row, (count, row.shape[1]))
    i = lax.broadcasted_iota(jnp.int32, wide.shape, 0)
    j = lax.broadcasted_iota(jnp.int32, wide.shape, 1)
    return jnp.sum(jnp.where(i == j, wide, 0.0), axis=1, keepdims=True)


def as_row(column, width):
    wide = jnp.broadcast_to(column, (column.shape[0], width))
    i = lax.broadcasted_iota(jnp.int32, wide.shape, 0)
    j = lax.broadcasted_iota(jnp.int32, wide.shape, 1)
    return jnp.sum(jnp.where(i == j, wide, 0.0), axis=0, keepdims=True)


def docs_column(starts_row, first, count):
    position = first + lax.broadcasted_iota(jnp.int32, (count, starts_row.shape[1]), 0)
    hit = jnp.where(starts_row <= position, 1.0, 0.0)
    return jnp.sum(hit, axis=1, keepdims=True)


def docs_row(starts_row, first, count):
    position = first + lax.broadcasted_iota(jnp.int32, (count, starts_row.shape[1]), 0)
    hit = jnp.where(starts_row <= position, 1.0, 0.0).astype(BF16)
    ones = jnp.ones((8, starts_row.shape[1]), BF16)
    return dot_last(ones, hit)[:1, :]


def state_kernel(
    head_size,
    offset_ref,
    y_ref,
    core_ref,
    stream_hbm,
    in_hbm,
    step_hbm,
    bias_hbm,
    rate_hbm,
    starts_hbm,
    summary_ref,
    first_ref,
    into_ref,
    factor_ref,
    stream_ref,
    in_ref,
    step_ref,
    bias_ref,
    rate_ref,
    starts_ref,
    arrived,
):
    pairs = (
        (step_hbm, step_ref),
        (bias_hbm, bias_ref),
        (rate_hbm, rate_ref),
        (starts_hbm, starts_ref),
        (in_hbm, in_ref),
        (stream_hbm, stream_ref),
    )
    copies = [
        pltpu.make_async_copy(source, target, arrived.at[number])
        for number, (source, target) in enumerate(pairs)
    ]
    for copy in copies:
        copy.start()
    heads, rows = step_ref.shape
    width = stream_ref.shape[1]
    spread = head_lanes(width, head_size)
    i = lax.broadcasted_iota(jnp.int32, (BLOCK, BLOCK), 0)
    j = lax.broadcasted_iota(jnp.int32, (BLOCK, BLOCK), 1)
    upper = jnp.where(i <= j, 1.0, 0.0)
    for copy in copies[:4]:
        copy.wait()
    offset = offset_ref[0]
    starts = starts_ref[...]
    docs = docs_column(starts, offset, rows)
    before = jnp.max(docs_column(starts, offset - 1, 8)[:1, :], axis=0, keepdims=True)
    raw = step_ref[...] + as_column(bias_ref[...], heads)
    step = jnp.maximum(raw, 0.0) + jnp.log1p(jnp.exp(-jnp.abs(raw)))
    log_decay = -step * as_column(rate_ref[...], heads)
    into, out_of, half, last = [], [], [], []
    for block in range(rows // BLOCK):
        cut = slice(block * BLOCK, (block + 1) * BLOCK)
        cumulative = jnp.dot(
            log_decay[:, cut], upper, precision=lax.Precision.HIGHEST, preferred_element_type=F32
        )
        end = cumulative[:, BLOCK - 1 :]
        middle = 0.5 * end
        into.append(step[:, cut] * jnp.exp(middle - cumulative))
        out_of.append(jnp.exp(cumulative - middle))
        half.append(jnp.exp(middle))
        last.append(end)
    ends = [docs[(b + 1) * BLOCK - 1 : (b + 1) * BLOCK, :] for b in range(rows // BLOCK)]
    joined_0 = jnp.where(ends[0] == before, 1.0, 0.0)
    joined_1 = jnp.where(ends[1] == ends[0], 1.0, 0.0)
    gate_0 = joined_0 * jnp.exp(last[0])
    gate_1 = joined_1 * jnp.exp(last[1])
    link = joined_0 * joined_1 * jnp.exp(last[0] + last[1])
    lane = lax.broadcasted_iota(jnp.int32, (heads, LANES), 1)
    constants = jnp.where(lane == 0, half[0], 0.0)
    constants = jnp.where(lane == 1, half[1], constants)
    constants = jnp.where(lane == 2, gate_0, constants)
    constants = jnp.where(lane == 3, gate_1, constants)
    nothing = jnp.zeros((PAD - heads, rows + LANES), F32)
    wide_in = jnp.concatenate([jnp.concatenate(into + [constants], axis=1), nothing], axis=0)
    wide_out = jnp.concatenate([jnp.concatenate(out_of + [constants], axis=1), nothing], axis=0)
    factor_ref[...] = two_parts(wide_out)
    into_parts = two_parts(wide_in)
    into_ref[...] = into_parts
    per_lane = dot_first(into_parts[:, :rows], spread)
    constant_rows = dot_first(into_parts[:, rows : rows + 8], spread)
    for copy in copies[4:]:
        copy.wait()
    states = []
    for block in range(rows // BLOCK):
        cut = slice(block * BLOCK, (block + 1) * BLOCK)
        scaled = (stream_ref[cut, :].astype(F32) * per_lane[cut, :]).astype(BF16)
        to_end = jnp.where(docs[cut, :] == ends[block], in_ref[cut, :].astype(F32), 0.0)
        states.append(constant_rows[block : block + 1, :] * dot_first(to_end.astype(BF16), scaled))
    first_ref[...] = states[0].astype(BF16)
    summary = constant_rows[3:4, :] * states[0] + states[1]
    high = link.astype(BF16).astype(F32)
    link_row = as_row(high, LANES) + pltpu.roll(as_row(link - high, LANES), PAD, 1)
    whole = jnp.concatenate(
        [summary, jnp.broadcast_to(link_row, (summary.shape[0], LANES))], axis=1
    ).astype(BF16)
    summary_ref[...] = whole


def block_terms(
    head_size,
    offset,
    block,
    stream_ref,
    gate_ref,
    in_ref,
    out_ref,
    into_ref,
    factor_ref,
    skip_ref,
    starts_ref,
):
    rows, width = stream_ref.shape
    heads = skip_ref.shape[1]
    step = rows // 4
    inner = block % (BLOCK // step)
    start = pl.multiple_of(block * step, step)
    origin = pl.multiple_of((block - inner) * step, BLOCK)
    here = pl.ds(start, step)
    whole = pl.ds(origin, BLOCK)
    starts = starts_ref[...]
    docs = docs_column(starts, offset + start, step)
    docs_across = docs_row(starts, offset + origin, BLOCK)
    before = jnp.max(docs_column(starts, offset + origin - 1, 8)[:1, :], axis=0, keepdims=True)
    spread = head_lanes(width, head_size)
    skip = jnp.concatenate(
        [as_column(skip_ref[...], heads), jnp.zeros((PAD - heads, 1), F32)], axis=0
    )
    skip_row = dot_first(two_parts(jnp.broadcast_to(skip, (PAD, LANES))), spread)[:1, :]
    scaled = stream_ref[whole, :].astype(F32) * dot_first(into_ref[:, whole], spread)
    own = out_ref[here, :]
    scores = dot_last(own, in_ref[whole, :])
    i = inner * step + lax.broadcasted_iota(jnp.int32, (step, BLOCK), 0)
    j = lax.broadcasted_iota(jnp.int32, (step, BLOCK), 1)
    live = (i >= j) & (docs == docs_across)
    weights = jnp.where(live, scores, 0.0).astype(BF16)
    per_lane = dot_first(factor_ref[:, here], spread)
    value = per_lane * dot(weights, scaled.astype(BF16)) + skip_row * stream_ref[here, :].astype(F32)
    gate = gate_ref[here, :].astype(F32)
    gate = gate / (1.0 + jnp.exp(-gate))
    joined = jnp.where(docs == before, own.astype(F32), 0.0).astype(BF16)
    return value * gate, per_lane * gate, joined


def block_hidden(base, slope, joined, state, gain):
    gated = base + slope * dot(joined, state)
    square = gated * gated
    total = square[:, :LANES]
    for lane in range(LANES, square.shape[1], LANES):
        total = total + square[:, lane : lane + LANES]
    return (gated * gain).astype(BF16), jnp.sum(jnp.transpose(total), axis=0, keepdims=True)


def ahead_kernel(head_size, offset_ref, y_ref, *refs):
    base_ref, slope_ref, joined_ref = refs[-3:]
    base_ref[...], slope_ref[...], joined_ref[...] = block_terms(
        head_size, offset_ref[0], y_ref[0] ^ 2, *refs[:-3]
    )


def link_lanes(links, width, head_size):
    lane = lax.broadcasted_iota(jnp.int32, (LANES, width), 0)
    spot = lax.broadcasted_iota(jnp.int32, (LANES, width), 1)
    head = jnp.where(lane >= PAD, lane - PAD, lane)
    first = head * head_size
    spread = jnp.where(
        (lane < 2 * PAD) & (spot >= first) & (spot < first + head_size), 1.0, 0.0
    ).astype(BF16)
    return dot(links, spread)


def combine_kernel(head_size, core_ref, own_ref, other_ref, pieces_ref):
    states, wide = own_ref.shape
    width = wide - LANES
    half = width // 2
    first_core = core_ref[0] == 0
    own = own_ref[...].astype(F32)
    other = other_ref[...].astype(F32)
    earlier = jnp.where(first_core, own, other)
    later = jnp.where(first_core, other, own)
    rate = link_lanes(later[:8, width:].astype(BF16), width, head_size)[:1, :]
    total = rate * earlier[:, :width] + later[:, :width]
    total = jnp.where(first_core, total[:, :half], total[:, half:])
    parts_a, parts_b = own[:8, width:], other[:8, width:]
    link = (parts_a + pltpu.roll(parts_a, LANES - PAD, 1)) * (
        parts_b + pltpu.roll(parts_b, LANES - PAD, 1)
    )
    lane = lax.broadcasted_iota(jnp.int32, link.shape, 1)
    heads = half // head_size
    link = jnp.where(first_core, link, pltpu.roll(link, LANES - heads, 1))
    link = jnp.where(lane < heads, link, 0.0)
    high = link.astype(BF16).astype(F32)
    link = high + pltpu.roll(link - high, PAD, 1)
    link = jnp.broadcast_to(link[:1, :], (states, LANES))
    pieces_ref[...] = jnp.concatenate([total, link], axis=1).astype(BF16).reshape(pieces_ref.shape)


def scan_kernel(head_size, pieces_ref, before_ref):
    chips, rows, wide = pieces_ref.shape
    width = wide - LANES
    per_lane = link_lanes(pieces_ref[:, 0, width:], width, head_size)
    state = jnp.zeros((rows, width), F32)
    for chip in range(chips):
        before_ref[chip] = state.astype(BF16)
        state = per_lane[chip : chip + 1, :] * state + pieces_ref[chip, :, :width].astype(F32)


def with_squares(piece, squares):
    width = piece.shape[1]
    high = squares.astype(BF16).astype(F32)
    row = jnp.concatenate(
        [high, squares - high, jnp.zeros((1, width - 2 * squares.shape[1]), F32)], axis=1
    )
    return jnp.concatenate(
        [piece.astype(BF16), jnp.broadcast_to(row, (8, width)).astype(BF16)], axis=0
    )


def squares_of(got_ref, step):
    row = got_ref[step:, :].astype(F32)[:1, :]
    return row[:, :step] + row[:, step : 2 * step]


def state_of(states_ref, block):
    states = states_ref.shape[0] // 2
    return states_ref[pl.ds(pl.multiple_of((block // 2) * states, states), states), :]


def far_kernel(
    head_size,
    y_ref,
    core_ref,
    before_ref,
    before_other_ref,
    other_ref,
    first_ref,
    factor_ref,
    base_ref,
    slope_ref,
    joined_ref,
    gain_ref,
    proj_ref,
    send_a_ref,
    send_b_ref,
    states_ref,
):
    width = base_ref.shape[1]
    states = other_ref.shape[0]
    rows = factor_ref.shape[1] - LANES
    spread = head_lanes(width, head_size)
    constant_rows = dot_first(factor_ref[:, rows:], spread)[:8, :]
    first_core = core_ref[0] == 0
    half_a = before_ref[...].reshape(states, width // 2).astype(F32)
    half_b = before_other_ref[...].reshape(states, width // 2).astype(F32)
    state = jnp.concatenate(
        [jnp.where(first_core, half_a, half_b), jnp.where(first_core, half_b, half_a)], axis=1
    )
    rate = link_lanes(other_ref[:8, width:], width, head_size)[:1, :]
    state = jnp.where(first_core, state, rate * state + other_ref[:, :width].astype(F32))
    states_ref[:states, :] = (constant_rows[:1, :] * state).astype(BF16)
    state = constant_rows[2:3, :] * state + first_ref[...].astype(F32)
    states_ref[states:, :] = (constant_rows[1:2, :] * state).astype(BF16)
    piece, squares = block_hidden(
        base_ref[...],
        slope_ref[...],
        joined_ref[...],
        state_of(states_ref, y_ref[0] ^ 2),
        gain_ref[...].reshape(1, width),
    )
    low = send_b_ref.shape[1]
    send_b_ref[...] = dot(piece, proj_ref[:, -low:]).astype(BF16)
    send_a_ref[...] = with_squares(dot(piece, proj_ref[:, :-low]), squares)


def near_kernel(head_size, offset_ref, y_ref, states_ref, gain_ref, proj_ref, *refs):
    send_a_ref, send_b_ref, hidden_ref, squares_ref = refs[-4:]
    step = refs[0].shape[0] // 4
    low = send_b_ref.shape[1]
    gain = gain_ref[...].reshape(1, -1)
    for number, block in enumerate((y_ref[0] ^ 3, y_ref[0] ^ 1)):
        terms = block_terms(head_size, offset_ref[0], block, *refs[:-4])
        piece, squares = block_hidden(*terms, state_of(states_ref, block), gain)
        hidden_ref[number * step : (number + 1) * step, :] = piece
        if number == 0:
            send_b_ref[...] = dot(piece, proj_ref[:, -low:]).astype(BF16)
            squares_ref[...] = squares
        else:
            send_a_ref[...] = with_squares(dot(piece, proj_ref[:, :-low]), squares)


def keep_kernel(head_size, offset_ref, y_ref, states_ref, gain_ref, proj_ref, hidden_ref, *refs):
    own_ref, via_a_ref, via_b_ref, squares_ref = refs[-4:]
    step = refs[0].shape[0] // 4
    low = via_b_ref.shape[1]
    via_a_ref[...] = dot(hidden_ref[:step, :], proj_ref[:, :-low])
    via_b_ref[...] = dot(hidden_ref[step:, :], proj_ref[:, -low:])
    terms = block_terms(head_size, offset_ref[0], y_ref[0], *refs[:-4])
    piece, squares = block_hidden(
        *terms, state_of(states_ref, y_ref[0]), gain_ref[...].reshape(1, -1)
    )
    squares_ref[...] = squares
    own_ref[...] = dot(piece, proj_ref[...])


def middle_kernel(squares_ref, via_a_ref, via_b_ref, got_a_ref, got_b_ref, send_a_ref, send_b_ref):
    step = via_a_ref.shape[0]
    squares = squares_ref[...] + squares_of(got_a_ref, step)
    send_a_ref[...] = with_squares(via_a_ref[...] + got_a_ref[:step, :].astype(F32), squares)
    send_b_ref[...] = (via_b_ref[...] + got_b_ref[...].astype(F32)).astype(BF16)


def last_kernel(
    channels,
    squares_ref,
    own_ref,
    near_a_ref,
    near_b_ref,
    far_a_ref,
    far_b_ref,
    out_hbm,
    out_ref,
    left,
):
    step, model = own_ref.shape
    edge = near_a_ref.shape[1]
    squares = squares_ref[...]
    squares = squares + squares_of(near_a_ref, step) + squares_of(far_a_ref, step)
    scale = as_column(lax.rsqrt(squares / channels + EPSILON), step)
    chunk = step // 4
    copies = []
    for number in range(4):
        cut = slice(number * chunk, (number + 1) * chunk)
        for near_ref, far_ref, low, high in (
            (near_a_ref, far_a_ref, 0, edge),
            (near_b_ref, far_b_ref, edge, model),
        ):
            total = (
                own_ref[cut, low:high]
                + near_ref[cut, :].astype(F32)
                + far_ref[cut, :].astype(F32)
            )
            out_ref[cut, low:high] = (total * scale[cut, :]).astype(BF16)
        here = pl.ds(number * chunk, chunk)
        copy = pltpu.make_async_copy(out_ref.at[here, :], out_hbm.at[here, :], left.at[number])
        copy.start()
        copies.append(copy)
    for copy in copies:
        copy.wait()


def call(kernel, out_shape, scalars, arrays, flops, limit, scratch=(), space=VMEM_SPEC, result=VMEM_SPEC):
    single = not isinstance(out_shape, (tuple, list))
    return pl.pallas_call(
        kernel,
        out_shape=out_shape,
        in_specs=[SMEM_SPEC] * len(scalars) + [space] * len(arrays),
        out_specs=result if single else [result] * len(out_shape),
        scratch_shapes=scratch,
        cost_estimate=pl.CostEstimate(flops=flops, bytes_accessed=4_000_000, transcendentals=0),
        compiler_params=pltpu.CompilerParams(vmem_limit_bytes=int(limit * 1024**2)),
    )(*scalars, *arrays)


def local(
    total_channels,
    stream,
    gate_input,
    in_coeff,
    out_coeff,
    step_raw,
    step_bias,
    decay_rate,
    skip_scale,
    norm_gain,
    out_proj,
    doc_starts,
):
    rows, width = stream.shape
    heads = step_raw.shape[0]
    head_size = width // heads
    states = in_coeff.shape[1]
    model = out_proj.shape[1]
    chips = lax.axis_size(CHIPS)
    core = lax.axis_index("seq_2").astype(jnp.int32)[None]
    y = lax.axis_index("head").astype(jnp.int32)[None]
    offset = (lax.axis_index(SEQ) * rows).astype(jnp.int32)[None]
    starts = doc_starts[None, :]
    shape = jax.ShapeDtypeStruct
    arrays = [
        pltpu.with_memory_space_constraint(a, pltpu.HBM)
        for a in (stream, in_coeff, step_raw, step_bias[None], decay_rate[None], starts)
    ]
    summary, first, into, factor = call(
        functools.partial(state_kernel, head_size),
        [
            shape((states, width + LANES), BF16),
            shape((states, width), BF16),
            shape((2 * PAD, rows + LANES), BF16),
            shape((2 * PAD, rows + LANES), BF16),
        ],
        [offset, y, core],
        arrays,
        2_000_000_000,
        24,
        [pltpu.VMEM(a.shape, a.dtype) for a in arrays] + [pltpu.SemaphoreType.DMA((len(arrays),))],
        HBM_SPEC,
    )
    other = lax.ppermute(summary, "seq_2", [(0, 1), (1, 0)])
    pieces = call(
        functools.partial(combine_kernel, head_size),
        shape((chips, states // chips, width // 2 + LANES), BF16),
        [core],
        [summary, other],
        200_000_000,
        8,
    )
    pieces = lax.all_to_all(pieces, CHIPS, 0, 0, tiled=True)
    prior = call(
        functools.partial(scan_kernel, head_size),
        shape((chips, states // chips, width // 2), BF16),
        [],
        [pieces],
        10_000_000_000,
        8,
    )
    incoming = lax.all_to_all(prior, CHIPS, 0, 0, tiled=True)
    incoming_other = lax.ppermute(incoming, "seq_2", [(0, 1), (1, 0)])
    step = rows // 4
    edge = model * 11 // 20
    rest = model - edge
    tokens = [
        stream,
        gate_input,
        in_coeff,
        out_coeff,
        into,
        factor,
        skip_scale[None],
        starts,
    ]
    base, slope, joined = call(
        functools.partial(ahead_kernel, head_size),
        [shape((step, width), F32), shape((step, width), F32), shape((step, states), BF16)],
        [offset, y],
        tokens,
        2_000_000_000,
        16,
    )
    send_a, send_b, ready = call(
        functools.partial(far_kernel, head_size),
        [
            shape((step + 8, edge), BF16),
            shape((step, rest), BF16),
            shape((2 * states, width), BF16),
        ],
        [y, core],
        [
            incoming,
            incoming_other,
            other,
            first,
            factor,
            base,
            slope,
            joined,
            norm_gain,
            out_proj,
        ],
        1_000_000_000,
        16,
    )
    pair_1 = [(i, i ^ 1) for i in range(4)]
    pair_3 = [(i, i ^ 3) for i in range(4)]
    got_a = lax.ppermute(send_a, "head", pair_1)
    got_b = lax.ppermute(send_b, "head", pair_3)
    send_a, send_b, hidden, via_squares = call(
        functools.partial(near_kernel, head_size),
        [
            shape((step + 8, edge), BF16),
            shape((step, rest), BF16),
            shape((2 * step, width), BF16),
            shape((1, step), F32),
        ],
        [offset, y],
        [ready, norm_gain, out_proj] + tokens,
        2_000_000_000,
        20,
    )
    near_a = lax.ppermute(send_a, "head", pair_1)
    near_b = lax.ppermute(send_b, "head", pair_3)
    own, via_a, via_b, squares = call(
        functools.partial(keep_kernel, head_size),
        [
            shape((step, model), F32),
            shape((step, edge), F32),
            shape((step, rest), F32),
            shape((1, step), F32),
        ],
        [offset, y],
        [ready, norm_gain, out_proj, hidden] + tokens,
        2_000_000_000,
        20,
    )
    send_a, send_b = call(
        middle_kernel,
        [shape((step + 8, edge), BF16), shape((step, rest), BF16)],
        [],
        [via_squares, via_a, via_b, got_a, got_b],
        1_000_000_000,
        8,
    )
    far_a = lax.ppermute(send_a, "head", pair_3)
    far_b = lax.ppermute(send_b, "head", pair_1)
    return call(
        functools.partial(last_kernel, total_channels),
        shape((step, model), BF16),
        [],
        [squares, own, near_a, near_b, far_a, far_b],
        1_000_000_000,
        8,
        [pltpu.VMEM((step, model), BF16), pltpu.SemaphoreType.DMA((4,))],
        VMEM_SPEC,
        HBM_SPEC,
    )


def solution(mesh):
    split = Mesh(
        mesh.devices.reshape(4, 8, 2, mesh.shape["head"]), ("seq_0", "seq_1", "seq_2", "head")
    )
    in_specs = (
        P(SEQ, "head"),
        P(SEQ, "head"),
        P(SEQ, None),
        P(SEQ, None),
        P("head", SEQ),
        P("head"),
        P("head"),
        P("head"),
        P("head"),
        P("head", None),
        P(),
    )
    out_specs = P(SEQ_HEAD, None)

    def whole(*args):
        step = functools.partial(local, float(args[0].shape[1]))
        return jax.shard_map(
            step, mesh=split, in_specs=in_specs, out_specs=out_specs, check_vma=False
        )(*args)

    return whole
```
